128 devices in a mesh: views: 32 (over x, y, core), heads: 4 (over z).
Axes of the slice: x: 4, y: 4, z: 4, core: 2. Of those that a mesh axis runs over, the one named last changes fastest.
Arguments:
- latents: bfloat16 [128, 256, 1024], P('views'), may hold values from -6 to 6
- norm_gain: float32 [1024], replicated, may hold values from 0.25 to 1.75
- w_qkv: bfloat16 [3, 1024, 1024], P(None, None, 'heads'), may hold values from -0.1875 to 0.1875
- w_out: bfloat16 [1024, 1024], P('heads'), may hold values from -0.1875 to 0.1875
- intersection: int32 [128, 2], replicated, may hold values 0 or 1
- match_block: int32 [32768, 1], P('views'), may hold values from 0 to 31; in each aligned block of 1024 rows (0 to 1023, 1024 to 2047, ...) at most 64 rows name the same one
- match_row: int32 [32768], P('views'), may hold values from 0 to 1023
- confidence: float32 [32768], P('views'), may hold values from 0.2 to 1
Outputs:
- refined: float32 [128, 256, 1024], P('views', None, 'heads')
The draws below stay inside these ranges and needn't reach their ends.
Inputs may be any that keep to these rules, and one draw needn't show every extreme that they name: `match_block`: among the rows of one device (1024 aligned rows), at most 64 name the same block, and some block is named by exactly 64 of them.
All inputs are finite; a program needn't handle non-finite values.
Results may differ from the reference program's by a relative error of at most 0.012.
The reference program's roundings to bfloat16 on the way (of `normed`, `attended`, `layer_out` and `fetched`) count: a program that leaves them out, or rounds other values in their place, can miss the bound.
Values may be sent and summed in bfloat16 or wider, within the bound.
A program may use at most 128 MiB of HBM per device.

```python
import math
import jax
import jax.numpy as jnp
import numpy as np
from jax import lax

D = 1024
HEADS = 16
TOK = 256
V_DEV = 4
WINDOW = 2
HEAD_DIM = 64
VIEWS = 128
ROWS = 32768
CAP = 64
N_VIEWS = 32
N_HEADS = 4


def draw_w_qkv(key, part):
    width = D
    limit = 6.0 / math.sqrt(width)
    pieces = jax.random.split(jax.random.fold_in(key, 7), 1)
    full = jax.random.normal(pieces[0], (3, width, width), jnp.float32) / math.sqrt(width)
    return jnp.clip(full, -limit, limit).astype(jnp.bfloat16)


def touch_ends(values, key, smallest, high):
    longest = values.shape.index(max(values.shape))
    spots = []
    for shift in (0, 1):
        where = [jax.random.randint(jax.random.fold_in(key, axis), (), 0, length) for axis, length in enumerate(values.shape)]
        where[longest] = (where[longest] + shift) % values.shape[longest]
        spots.append(tuple(where))
    return values.at[spots[0]].set(smallest).at[spots[1]].set(high)


def levels(own_key, dims, shards, low, top_value):
    loudness, own = 1.0, jax.random.fold_in(own_key, 6)
    for dim, shards_of in shards:
        draws = jnp.exp(jax.random.uniform(jax.random.fold_in(own, dim), (shards_of,), jnp.float32, low / len(shards), top_value / len(shards)))
        loudness = loudness * jnp.repeat(draws, dims[dim] // shards_of).reshape([-1 if axis == dim else 1 for axis in range(len(dims))])
    return loudness


def shared_out(stream_key, own, number, rows, amount, top, most, lean):
    ranking = jax.random.permutation(stream_key, amount)
    heavy_load, ordinary = shares(amount, rows * top, most, lean, True), shares(amount, rows * top, most, lean, False)
    places = jnp.arange(amount)

    def named(tallies, turn):
        used = int((tallies > 0).sum())
        fixed = max(1, used // 4)
        shifted = fixed + (places - fixed + turn * (used - fixed)) % max(1, amount - fixed)
        return jnp.zeros((amount,), jnp.int32).at[ranking[jnp.where(places < fixed, places, shifted)]].set(jnp.asarray(tallies, jnp.int32))

    tallies = jnp.where(number % 4 == 0, named(heavy_load, number // 4), named(ordinary, number - number // 4 - 1))
    mixed = jax.random.permutation(jax.random.fold_in(own, 3), amount)
    source_of, receiver = mixed[0:amount // 2 * 2:2], mixed[1:amount // 2 * 2:2]
    room = jnp.minimum(tallies[source_of] - 1, most - tallies[receiver]) // 2
    room = jnp.where((source_of == ranking[0]) | (receiver == ranking[0]) | (tallies[receiver] == 0), 0, jnp.maximum(room, 0))
    shifted = jax.random.randint(jax.random.fold_in(own, 4), (amount // 2,), 0, 1 << 20) % (room + 1)
    tallies = tallies.at[source_of].add(-shifted).at[receiver].add(shifted)
    items = jnp.searchsorted(jnp.cumsum(tallies), jnp.arange(rows * top), side="right").astype(jnp.int32)
    table = items.reshape(top, rows).T
    table = table[jax.random.permutation(jax.random.fold_in(own, 1), rows)]
    turn = jax.random.randint(jax.random.fold_in(own, 2), (rows, 1), 0, top)
    return jnp.take_along_axis(table, (jnp.arange(top)[None, :] + turn) % top, axis=1)


def shares(count, total, most, lean, full):
    weights = [(1 << 20) // math.isqrt(rank ** lean) + 1 for rank in range(1, count + 1)]
    largest = most if full else min(most, max(-(-total // count), total * weights[0] // sum(weights)))
    least = 1 if total - largest >= count - 1 else 0
    given, rest = [largest] + [least] * (count - 1), total - largest - least * (count - 1)
    while rest > 0:
        free = [i for i in range(1, count) if given[i] < largest] or [i for i in range(1, count) if given[i] < most]
        pool, left = sum([weights[i] for i in free]), rest
        for i in free:
            more = min(most - given[i], max(1, left * weights[i] // pool), rest)
            given[i] = given[i] + more
            rest = rest - more
    return np.array(given)


def bell_draw(stream_key, extent, scale, bound, cuts=(), kind=jnp.bfloat16):
    loudness = levels(stream_key, extent, cuts, -0.22, 0.18) if cuts else 1.0
    drawn = jax.random.normal(stream_key, extent, jnp.float32) * scale * loudness
    return jnp.minimum(jnp.maximum(drawn, -bound), bound).astype(kind)


def setup_inputs(seed: int = 0) -> dict:
    streams_of = jax.random.split(jax.random.key(seed), 9)
    latents = bell_draw(streams_of[0], (VIEWS, TOK, D), 1.0, 6.0, ((0, 32),))
    norm_gain = jnp.clip(1.0 + 0.15 * jax.random.normal(streams_of[1], (D,), jnp.float32), 0.25, 1.75)
    w_qkv = draw_w_qkv(jax.random.fold_in(streams_of[8], 71), 0)
    w_out = bell_draw(streams_of[3], (D, D), D ** -0.5, 0.1875, ((0, 4),))
    intersection = touch_ends((jax.random.randint(streams_of[4], (VIEWS, WINDOW), 0, 3) < 2).astype(jnp.int32), jax.random.fold_in(streams_of[4], 1), 0, 1)
    match_block_keys = jax.random.split(jax.random.fold_in(streams_of[5], 1), ROWS // (V_DEV * TOK))
    match_block_turns = jax.random.permutation(jax.random.fold_in(streams_of[5], 3), ROWS // (V_DEV * TOK))
    match_block = jax.vmap(lambda own, number: shared_out(jax.random.fold_in(streams_of[5], 2), own, number, V_DEV * TOK, N_VIEWS, 1, CAP, 2))(match_block_keys, match_block_turns).reshape((ROWS, 1))
    match_row = touch_ends(jax.random.randint(streams_of[6], (ROWS,), 0, V_DEV * TOK), jax.random.fold_in(streams_of[6], 1), 0, (V_DEV * TOK) - 1).astype(jnp.int32)
    confidence = jnp.clip(jnp.exp(math.log(1.0) - 1.609438 * jax.random.uniform(streams_of[7], (ROWS,), jnp.float32) ** levels(streams_of[7], (ROWS,), ((0, 32),), -0.2, 0.2)), 0.2, 1.0)
    return dict(latents=latents, norm_gain=norm_gain, w_qkv=w_qkv, w_out=w_out, intersection=intersection, match_block=match_block, match_row=match_row, confidence=confidence)


neg_large = -1e+30
coupling = 0.5
epsilon = 1e-06

def partial_block(queries, keys, values):
    query_heads = queries.reshape(TOK, HEADS, HEAD_DIM).astype(jnp.float32)
    key_heads = keys.reshape(TOK, HEADS, HEAD_DIM).astype(jnp.float32)
    value_heads = values.reshape(TOK, HEADS, HEAD_DIM).astype(jnp.float32)
    scores = jnp.einsum('qhd,khd->hqk', query_heads, key_heads) * HEAD_DIM ** (-0.5)
    maximum = lax.optimization_barrier(jnp.max(scores, axis=-1))
    weights = jnp.exp(scores - maximum[..., None])
    totals = lax.optimization_barrier(jnp.sum(weights, axis=-1))
    rounded = weights.astype(jnp.bfloat16).astype(jnp.float32)
    numerator = jnp.einsum('hqk,khd->hqd', rounded, value_heads)
    return (maximum, totals, numerator)

def merge_into(running, piece_part, present):
    maximum, totals, numerator = running
    other_max, other_tot, other_num = piece_part
    other_max = jnp.where(present > 0, other_max, neg_large)
    highest = jnp.maximum(maximum, other_max)
    old_scale = jnp.exp(maximum - highest)
    new_scale = jnp.exp(other_max - highest) * present
    return (highest, totals * old_scale + other_tot * new_scale, numerator * old_scale[..., None] + other_num * new_scale[..., None])

def reference(latents, norm_gain, w_qkv, w_out, intersection, match_block, match_row, confidence):
    wide_latents = latents.astype(jnp.float32)
    mean_square = lax.optimization_barrier(jnp.mean(wide_latents * wide_latents, axis=-1, keepdims=True))
    normed = (wide_latents * lax.rsqrt(mean_square + epsilon) * norm_gain).astype(jnp.bfloat16)
    flat_normed = normed.reshape(ROWS, D)
    all_queries = jnp.dot(flat_normed, w_qkv[0], preferred_element_type=jnp.float32).astype(jnp.bfloat16).reshape(VIEWS, TOK, D)
    all_keys = jnp.dot(flat_normed, w_qkv[1], preferred_element_type=jnp.float32).astype(jnp.bfloat16).reshape(VIEWS, TOK, D)
    all_values = jnp.dot(flat_normed, w_qkv[2], preferred_element_type=jnp.float32).astype(jnp.bfloat16).reshape(VIEWS, TOK, D)

    def view_attention(view_index):
        queries = all_queries[view_index]
        running = partial_block(queries, all_keys[view_index], all_values[view_index])
        for offset in range(WINDOW):
            forward = (view_index + offset + 1) % VIEWS
            present = intersection[view_index, offset].astype(jnp.float32)
            running = merge_into(running, partial_block(queries, all_keys[forward], all_values[forward]), present)
        for offset in range(WINDOW):
            backward = (view_index - offset - 1) % VIEWS
            present = intersection[backward, offset].astype(jnp.float32)
            running = merge_into(running, partial_block(queries, all_keys[backward], all_values[backward]), present)
        maximum, totals, numerator = running
        result = numerator / totals[..., None]
        return jnp.transpose(result, (1, 0, 2)).reshape(TOK, D).astype(jnp.bfloat16)
    attended = lax.map(view_attention, jnp.arange(VIEWS, dtype=jnp.int32)).reshape(ROWS, D)
    group_width = D // N_HEADS
    projected = jnp.zeros((ROWS, D), jnp.float32)
    for head_group in range(N_HEADS):
        group_part = jnp.dot(attended[:, head_group * group_width:(head_group + 1) * group_width], w_out[head_group * group_width:(head_group + 1) * group_width], preferred_element_type=jnp.float32).astype(jnp.bfloat16)
        group_part = lax.optimization_barrier(group_part)
        projected = projected + group_part.astype(jnp.float32)
    layer_out = (latents.reshape(ROWS, D).astype(jnp.float32) + projected).astype(jnp.bfloat16)
    layer_out = lax.optimization_barrier(layer_out)
    target_rows = (match_block[:, 0] * (V_DEV * TOK) + match_row).astype(jnp.int32)
    fetched = layer_out[target_rows].astype(jnp.float32)
    layer_wide = layer_out.astype(jnp.float32)
    refined = layer_wide + coupling * confidence[:, None] * (fetched - layer_wide)
    return refined.astype(jnp.float32).reshape(VIEWS, TOK, D)
```

```python
import functools

import jax
import jax.numpy as jnp
from jax import lax
from jax.experimental import pallas as pl
from jax.experimental.pallas import tpu as pltpu
from jax.sharding import PartitionSpec as P

MESH = pl.DeviceIdType.MESH
F32, BF16, I32 = jnp.float32, jnp.bfloat16, jnp.int32
EPSILON = 1e-06
COUPLING = 0.5
HEAD_DIM = 64
ORDER = (1, 2, 0, 3)


def dot(a, b):
    return jnp.dot(a, b, preferred_element_type=F32)


def dot_nt(a, b):
    return lax.dot_general(a, b, (((1,), (1,)), ((), ())), preferred_element_type=F32)


def kernel(
    nv, views_total, cap,
    lat, gain, wqkv, wout, inter, mb, mr, conf,
    out,
    kv, q, att, wo, lay, gsel, fsel, idxs, reqo, reqi, rows, reps,
    kv_s, kv_r, wo_s, wo_r, at_s, at_r, fw_s, fw_r, rq_s, rq_r, rp_s, rp_r,
):
    nl, tok, width = lat.shape
    sub = wqkv.shape[2]
    half = tok // 2
    me = lax.axis_index("views")
    z = lax.axis_index("heads")
    up, down, far = lax.rem(z + 1, 4), lax.rem(z + 3, 4), lax.rem(z + 2, 4)
    nxt, prv = lax.rem(me + 1, nv), lax.rem(me + nv - 1, nv)

    def remote(src, dst, send, recv, device):
        return pltpu.make_async_remote_copy(
            src_ref=src, dst_ref=dst, send_sem=send, recv_sem=recv,
            device_id=device, device_id_type=MESH,
        )

    barrier = pltpu.get_barrier_semaphore()

    def greet(k, carry):
        pl.semaphore_signal(
            barrier, inc=1, device_id=(lax.rem(me + k, nv), z), device_id_type=MESH
        )
        return carry

    lax.fori_loop(1, nv, greet, 0)
    for other in (up, down, far):
        pl.semaphore_signal(barrier, inc=1, device_id=(me, other), device_id_type=MESH)

    def kv_copy(i):
        slot, target = ((nl + 2 + i, prv) if i < 2 else (i - 2, nxt))
        return remote(kv.at[2 + i], kv.at[slot], kv_s.at[i], kv_r.at[i], (target, z))

    def wo_copy(rel):
        target = (z, up, far, down)[rel]
        cols = pl.ds(pl.multiple_of(target * sub, sub), sub)
        return remote(wout.at[:, cols], wo.at[rel], wo_s.at[rel], wo_r.at[rel], (me, target))

    def att_copy(i, way):
        return remote(
            att.at[i, 0], att.at[i, (1, 3)[way]], at_s.at[i, way], at_r.at[i, way],
            (me, (up, down)[way]),
        )

    def fwd_copy(i, way):
        part = pl.ds(way * half, half)
        return remote(
            att.at[i, (1, 3)[way], part], att.at[i, 2, part], fw_s.at[i, way], fw_r.at[i, way],
            (me, (up, down)[way]),
        )

    def req_copy(k):
        return remote(reqo.at[k], reqi.at[k], rq_s.at[k], rq_r.at[k], (lax.rem(me + k, nv), z))

    def rep_copy(k):
        return remote(
            rows.at[k], reps.at[k], rp_s.at[k], rp_r.at[k], (lax.rem(me + nv - k, nv), z)
        )

    for n, i in enumerate((3, 0, 1, 2)):
        wide = lat[i].astype(F32)
        mean_square = jnp.mean(wide * wide, axis=-1, keepdims=True)
        x = (wide * lax.rsqrt(mean_square + EPSILON) * gain[...]).astype(BF16)
        kv[2 + i, :, :sub] = dot(x, wqkv[1]).astype(BF16)
        kv[2 + i, :, sub:] = dot(x, wqkv[2]).astype(BF16)
        q[i] = (dot(x, wqkv[0]).astype(BF16).astype(F32) * HEAD_DIM ** (-0.5)).astype(BF16)
        if n == 0:
            pl.semaphore_wait(barrier, nv + 2)
            for rel in (1, 2, 3):
                wo_copy(rel).start()
        kv_copy(i).start()

    rel_block = mb[...] - me
    rel_block = jnp.where(rel_block < 0, rel_block + nv, rel_block)
    wanted = mr[...]
    lanes = mb.shape[1]
    block_iota = lax.broadcasted_iota(I32, (nv, lanes), 0)
    slot_iota = lax.broadcasted_iota(I32, (lanes, lanes), 0)
    before = (slot_iota < lax.broadcasted_iota(I32, (lanes, lanes), 1)).astype(F32).astype(BF16)
    base = jnp.zeros((nv, 1), F32)
    digits = jnp.zeros((2 * nv, lanes), F32)
    for c in range(mb.shape[0]):
        onehot = (rel_block[c : c + 1] == block_iota).astype(F32)
        earlier = dot(onehot.astype(BF16), before) + base
        slot = jnp.sum(onehot * earlier, axis=0, keepdims=True)
        base = base + jnp.sum(onehot, axis=1, keepdims=True)
        idxs[c : c + 1, :] = rel_block[c : c + 1].astype(F32) * cap + slot
        is_slot = (slot.astype(I32) == slot_iota).astype(F32).astype(BF16)
        row = wanted[c : c + 1]
        high, low = (row >> 5).astype(F32), (row & 31).astype(F32)
        both = jnp.concatenate([onehot * high, onehot * low], axis=0).astype(BF16)
        digits = digits + dot_nt(both, is_slot)
    requests = (digits[:nv] * 32.0 + digits[nv:]).astype(I32)
    for k in range(nv):
        reqo[k] = jnp.broadcast_to(requests[k : k + 1], reqo.shape[1:])
    reqi[0] = jnp.broadcast_to(requests[0:1], reqo.shape[1:])

    def send_request(k, carry):
        req_copy(k).start()
        return carry

    lax.fori_loop(1, nv, send_request, 0)

    lane = lax.broadcasted_iota(I32, (1, 2 * HEAD_DIM), 1)
    first = lane < HEAD_DIM

    def attend(i):
        a = me * nl + i
        bias = []
        for j in range(5):
            d = j - 2
            if d == 0:
                bias.append(None)
            else:
                source = a if d > 0 else lax.rem(a + d + views_total, views_total)
                present = inter[source * 2 + (abs(d) - 1)]
                bias.append((present.astype(F32) - 1.0) * 1e30)
        for t in range(sub // (2 * HEAD_DIM)):
            k_cols = slice(2 * HEAD_DIM * t, 2 * HEAD_DIM * (t + 1))
            v_cols = slice(sub + 2 * HEAD_DIM * t, sub + 2 * HEAD_DIM * (t + 1))
            pair = q[i, :, k_cols]
            done = []
            for mine in (first, jnp.logical_not(first)):
                query = jnp.where(mine, pair, jnp.zeros_like(pair))
                scores = []
                for j in range(5):
                    s = dot_nt(query, kv[i + j, :, k_cols])
                    scores.append(s if bias[j] is None else s + bias[j])
                top = functools.reduce(jnp.maximum, scores)
                top = jnp.max(top, axis=-1, keepdims=True)
                numer, total = None, None
                for j in range(5):
                    p = jnp.exp(scores[j] - top)
                    total = p if total is None else total + p
                    part = dot(p.astype(BF16), kv[i + j, :, v_cols])
                    numer = part if numer is None else numer + part
                total = jnp.sum(total, axis=-1, keepdims=True)
                done.append(numer / total)
            att[i, 0, :, k_cols] = jnp.where(first, done[0], done[1]).astype(BF16)

    def forward(i):
        for way in (0, 1):
            att_copy(i, way).wait_recv()
            fwd_copy(i, way).start()

    for n, i in enumerate(ORDER):
        if n == 0:
            kv_copy(3).wait_recv()
        elif n == 1:
            kv_copy(0).wait_recv()
        elif n == 2:
            kv_copy(2).wait_recv()
        else:
            kv_copy(1).wait_recv()
        attend(i)
        for way in (0, 1):
            att_copy(i, way).start()
        if n > 0:
            forward(ORDER[n - 1])

    n_slots = nv * cap
    places = jnp.transpose(idxs[...])
    for c in range(mb.shape[0]):
        place = places[:, c : c + 1].astype(I32)
        hit = place == lax.broadcasted_iota(I32, (lanes, n_slots), 1)
        fsel[lanes * c : lanes * (c + 1), :] = hit.astype(F32).astype(BF16)

    def take_request(k, carry):
        req_copy(k).wait()
        return carry

    lax.fori_loop(1, nv, take_request, 0)
    asked = jnp.transpose(reqi[:, 0, :])
    for k in range(nv):
        hit = asked[:cap, k : k + 1] == lax.broadcasted_iota(I32, (cap, nl * tok), 1)
        gsel[cap * k : cap * (k + 1), :] = hit.astype(F32).astype(BF16)

    forward(ORDER[-1])

    for rel in (1, 2, 3):
        wo_copy(rel).wait()

    own = pl.ds(pl.multiple_of(z * sub, sub), sub)
    for i in ORDER:
        for way in (0, 1):
            fwd_copy(i, way).wait_recv()
        proj = dot(att[i, 0], wout[:, own]).astype(BF16).astype(F32)
        for rel in (1, 2, 3):
            proj = proj + dot(att[i, rel], wo[rel]).astype(BF16).astype(F32)
        lay[tok * i : tok * (i + 1), :] = (lat[i, :, own].astype(F32) + proj).astype(BF16)

    group = 8
    for g in range(nv // group):
        picked = dot(gsel[group * cap * g : group * cap * (g + 1), :], lay[...]).astype(BF16)
        picked = picked.reshape(group, cap, sub)
        rows[group * g : group * (g + 1)] = picked
        if g == 0:
            reps[0] = picked[0]

        def send_reply(k, carry):
            rep_copy(k).start()
            return carry

        lax.fori_loop(max(1, group * g), group * (g + 1), send_reply, 0)

    for g in range(nv // group):

        def take_reply(k, carry):
            rep_copy(k).wait()
            return carry

        lax.fori_loop(max(1, group * g), group * (g + 1), take_reply, 0)
        block = reps[group * g : group * (g + 1)].reshape(group * cap, sub)
        part = dot(fsel[:, group * cap * g : group * cap * (g + 1)], block)
        if g == 0:
            out[...] = part
        else:
            out[...] += part

    weight = COUPLING * jnp.transpose(conf[...])
    for c in range(mb.shape[0]):
        here = slice(lanes * c, lanes * (c + 1))
        mine = lay[here, :].astype(F32)
        out[here, :] = mine + weight[:, c : c + 1] * (out[here, :] - mine)

    for i in range(nl):
        kv_copy(i).wait_send()
        for way in (0, 1):
            att_copy(i, way).wait_send()
            fwd_copy(i, way).wait_send()


def per_device(nv, latents, norm_gain, w_qkv, w_out, intersection, match_block, match_row, confidence):
    nl, tok, width = latents.shape
    sub = w_qkv.shape[2]
    rows = nl * tok
    cap = 2 * rows // nv
    vmem = pl.BlockSpec(memory_space=pltpu.VMEM)
    smem = pl.BlockSpec(memory_space=pltpu.SMEM)
    dma = pltpu.SemaphoreType.DMA
    lanes = 128
    result = pl.pallas_call(
        functools.partial(kernel, nv, nl * nv, cap),
        out_shape=jax.ShapeDtypeStruct((rows, sub), F32),
        in_specs=[vmem, vmem, vmem, vmem, smem, vmem, vmem, vmem],
        out_specs=vmem,
        scratch_shapes=[
            pltpu.VMEM((nl + 4, tok, 2 * sub), BF16),
            pltpu.VMEM((nl, tok, sub), BF16),
            pltpu.VMEM((nl, 4, tok, sub), BF16),
            pltpu.VMEM((4, sub, sub), BF16),
            pltpu.VMEM((rows, sub), BF16),
            pltpu.VMEM((nv * cap, rows), BF16),
            pltpu.VMEM((rows, nv * cap), BF16),
            pltpu.VMEM((rows // lanes, lanes), F32),
            pltpu.VMEM((nv, 8, lanes), I32),
            pltpu.VMEM((nv, 8, lanes), I32),
            pltpu.VMEM((nv, cap, sub), BF16),
            pltpu.VMEM((nv, cap, sub), BF16),
            dma((nl,)), dma((nl,)), dma((4,)), dma((4,)),
            dma((nl, 2)), dma((nl, 2)), dma((nl, 2)), dma((nl, 2)),
            dma((nv,)), dma((nv,)), dma((nv,)), dma((nv,)),
        ],
        compiler_params=pltpu.CompilerParams(
            collective_id=0, has_side_effects=True, vmem_limit_bytes=60 * 1024 * 1024
        ),
    )(
        latents,
        norm_gain.reshape(1, width),
        w_qkv,
        w_out,
        intersection.reshape(-1),
        match_block.reshape(rows // lanes, lanes),
        match_row.reshape(rows // lanes, lanes),
        confidence.reshape(rows // lanes, lanes),
    )
    return result.reshape(nl, tok, sub)


def solution(mesh):
    in_specs = (
        P("views", None, None),
        P(),
        P(None, None, "heads"),
        P("heads", None),
        P(),
        P("views", None),
        P("views"),
        P("views"),
    )
    out_specs = P("views", None, "heads")
    return jax.shard_map(
        functools.partial(per_device, mesh.shape["views"]),
        mesh=mesh, in_specs=in_specs, out_specs=out_specs, check_vma=False,
    )
```

```python
import functools

import jax
import jax.numpy as jnp
from jax import lax
from jax.experimental import pallas as pl
from jax.experimental.pallas import tpu as pltpu
from jax.sharding import PartitionSpec as P

MESH = pl.DeviceIdType.MESH
F32, BF16, I32 = jnp.float32, jnp.bfloat16, jnp.int32
EPSILON = 1e-06
COUPLING = 0.5
HEAD_DIM = 64
ORDER = (1, 2, 0, 3)
SIDE = 4


def ring_steps(d):
    return min(d, SIDE - d)


PLACES = sorted(
    ((dx, dy, dc) for dx in range(SIDE) for dy in range(SIDE) for dc in range(2)),
    key=lambda p: (-ring_steps(p[0]) - ring_steps(p[1]), -p[2]),
)
PICK_GROUPS = ((0, 4), (4, 8), (8, 16), (16, 24), (24, 32))
TAKE_GROUPS = ((0, 8), (8, 16), (16, 24), (24, 32))


def dot(a, b):
    return jnp.dot(a, b, preferred_element_type=F32)


def dot_nt(a, b):
    return lax.dot_general(a, b, (((1,), (1,)), ((), ())), preferred_element_type=F32)


def scope(name):
    return jax.named_scope(name)


def kernel(
    nv, views_total, cap,
    lat_h, gain_h, wqkv_h, wout_h, inter_h, mb_h, mr_h,
    lay_out, got_out,
    lat, gain, wqkv, wout, inter, mb, mr,
    kv, q, att, wo, part_s, part_r, lay, gsel, fsel, idxs, reqo, reqi, rows, reps, acc, got,
    in_sem, out_sem, kv_s, kv_r, wo_s, wo_r, at_s, at_r, pt_s, pt_r, rq_s, rq_r, rp_s, rp_r,
):
    nl, tok, width = lat.shape
    sub = wqkv.shape[2]
    me = lax.axis_index("views")
    z = lax.axis_index("heads")
    odd = lax.rem(z, 2)
    pair, opp = z + 1 - 2 * odd, lax.rem(z + 3 + 2 * odd, 4)
    pair_opp = lax.rem(pair + 3 + 2 * (1 - odd), 4)
    nxt, prv = lax.rem(me + 1, nv), lax.rem(me + nv - 1, nv)
    px, py, pc = me // (2 * SIDE), lax.rem(me // 2, SIDE), lax.rem(me, 2)

    def away(o, sign):
        dx, dy, dc = PLACES[o]
        bx = lax.rem(px + (dx if sign > 0 else SIDE - dx), SIDE)
        by = lax.rem(py + (dy if sign > 0 else SIDE - dy), SIDE)
        return bx * (2 * SIDE) + by * 2 + lax.rem(pc + dc, 2)

    def load(n, src, dst):
        copy = pltpu.make_async_copy(src, dst, in_sem.at[n])
        copy.start()
        return copy

    in_gain = load(0, gain_h, gain)
    in_lat = {3: load(1, lat_h.at[3], lat.at[3])}
    in_k = load(2, wqkv_h.at[1], wqkv.at[1])
    in_v = load(3, wqkv_h.at[2], wqkv.at[2])
    in_q = load(4, wqkv_h.at[0], wqkv.at[0])
    in_wout = load(5, wout_h, wout)
    for i in (0, 1, 2):
        in_lat[i] = load(6 + i, lat_h.at[i], lat.at[i])
    in_small = [load(9, mb_h, mb), load(10, mr_h, mr), load(11, inter_h, inter)]

    def remote(src, dst, send, recv, device):
        return pltpu.make_async_remote_copy(
            src_ref=src, dst_ref=dst, send_sem=send, recv_sem=recv,
            device_id=device, device_id_type=MESH,
        )

    barrier = pltpu.get_barrier_semaphore()

    def greet(k, carry):
        pl.semaphore_signal(
            barrier, inc=1, device_id=(lax.rem(me + k, nv), z), device_id_type=MESH
        )
        return carry

    lax.fori_loop(1, nv, greet, 0)
    for other in (pair, opp):
        pl.semaphore_signal(barrier, inc=1, device_id=(me, other), device_id_type=MESH)

    def kv_copy(i):
        slot, target = ((nl + 2 + i, prv) if i < 2 else (i - 2, nxt))
        return remote(kv.at[2 + i], kv.at[slot], kv_s.at[i], kv_r.at[i], (target, z))

    def wo_copy(n):
        cols = pl.ds(pl.multiple_of((pair, pair_opp)[n] * sub, sub), sub)
        return remote(wout.at[:, cols], wo.at[n], wo_s.at[n], wo_r.at[n], (me, pair))

    def att_copy(i):
        return remote(att.at[i, 0], att.at[i, 1], at_s.at[i], at_r.at[i], (me, pair))

    def part_copy(i):
        return remote(part_s.at[i], part_r.at[i], pt_s.at[i], pt_r.at[i], (me, opp))

    def req_copy(o):
        return remote(reqo.at[o], reqi.at[o], rq_s.at[o], rq_r.at[o], (away(o, 1), z))

    def rep_copy(o):
        return remote(rows.at[o], reps.at[o], rp_s.at[o], rp_r.at[o], (away(o, -1), z))

    in_gain.wait()
    for n, i in enumerate((3, 0, 1, 2)):
        with scope(f"proj{n}"):
            in_lat[i].wait()
            wide = lat[i].astype(F32)
            mean_square = jnp.mean(wide * wide, axis=-1, keepdims=True)
            x = (wide * lax.rsqrt(mean_square + EPSILON) * gain[...]).astype(BF16)
            if n == 0:
                in_k.wait()
            kv[2 + i, :, :sub] = dot(x, wqkv[1]).astype(BF16)
            if n == 0:
                in_v.wait()
            kv[2 + i, :, sub:] = dot(x, wqkv[2]).astype(BF16)
            if n == 0:
                in_q.wait()
            q[i] = (dot(x, wqkv[0]).astype(BF16).astype(F32) * HEAD_DIM ** (-0.5)).astype(BF16)
        if n == 0:
            with scope("greeted"):
                pl.semaphore_wait(barrier, nv + 1)
        kv_copy(i).start()
        if n == 0:
            in_wout.wait()
            for k in (0, 1):
                wo_copy(k).start()

    with scope("prep"):
        for copy in in_small:
            copy.wait()
        named = mb[...]
        rel = (((named >> 3) - px) & 3) * 8 + ((((named >> 1) & 3) - py) & 3) * 2 + ((named - pc) & 1)
        place = jnp.zeros_like(rel)
        for o, (dx, dy, dc) in enumerate(PLACES):
            place = jnp.where(rel == dx * 8 + dy * 2 + dc, o, place)
        wanted = mr[...]
        lanes = mb.shape[1]
        block_iota = lax.broadcasted_iota(I32, (nv, lanes), 0)
        slot_iota = lax.broadcasted_iota(I32, (lanes, lanes), 0)
        before = (slot_iota < lax.broadcasted_iota(I32, (lanes, lanes), 1)).astype(F32).astype(BF16)
        base = jnp.zeros((nv, 1), F32)
        digits = jnp.zeros((2 * nv, lanes), F32)
        for c in range(mb.shape[0]):
            onehot = (place[c : c + 1] == block_iota).astype(F32)
            earlier = dot(onehot.astype(BF16), before) + base
            slot = jnp.sum(onehot * earlier, axis=0, keepdims=True)
            base = base + jnp.sum(onehot, axis=1, keepdims=True)
            idxs[c : c + 1, :] = place[c : c + 1].astype(F32) * cap + slot
            is_slot = (slot.astype(I32) == slot_iota).astype(F32).astype(BF16)
            row = wanted[c : c + 1]
            high, low = (row >> 5).astype(F32), (row & 31).astype(F32)
            both = jnp.concatenate([onehot * high, onehot * low], axis=0).astype(BF16)
            digits = digits + dot_nt(both, is_slot)
        requests = (digits[:nv] * 32.0 + digits[nv:]).astype(I32)
        for k in range(nv):
            reqo[k] = jnp.broadcast_to(requests[k : k + 1], reqo.shape[1:])
        reqi[nv - 1] = jnp.broadcast_to(requests[nv - 1 : nv], reqo.shape[1:])
        for o in range(nv - 1):
            req_copy(o).start()

    lane = lax.broadcasted_iota(I32, (1, 2 * HEAD_DIM), 1)
    first = lane < HEAD_DIM

    def attend(i):
        a = me * nl + i
        bias = []
        for j in range(5):
            d = j - 2
            if d == 0:
                bias.append(None)
            else:
                source = a if d > 0 else lax.rem(a + d + views_total, views_total)
                present = inter[abs(d) - 1, source]
                bias.append((present.astype(F32) - 1.0) * 1e30)
        for t in range(sub // (2 * HEAD_DIM)):
            k_cols = slice(2 * HEAD_DIM * t, 2 * HEAD_DIM * (t + 1))
            v_cols = slice(sub + 2 * HEAD_DIM * t, sub + 2 * HEAD_DIM * (t + 1))
            both = q[i, :, k_cols]
            done = []
            for mine in (first, jnp.logical_not(first)):
                query = jnp.where(mine, both, jnp.zeros_like(both))
                scores = []
                for j in range(5):
                    s = dot_nt(query, kv[i + j, :, k_cols])
                    scores.append(s if bias[j] is None else s + bias[j])
                top = functools.reduce(jnp.maximum, scores)
                top = jnp.max(top, axis=-1, keepdims=True)
                numer, total = None, None
                for j in range(5):
                    p = jnp.exp(scores[j] - top)
                    total = p if total is None else total + p
                    part = dot(p.astype(BF16), kv[i + j, :, v_cols])
                    numer = part if numer is None else numer + part
                total = jnp.sum(total, axis=-1, keepdims=True)
                done.append(numer / total)
            att[i, 0, :, k_cols] = jnp.where(first, done[0], done[1]).astype(BF16)

    own = pl.ds(pl.multiple_of(z * sub, sub), sub)
    theirs = pl.ds(pl.multiple_of(opp * sub, sub), sub)

    def rounded(a, b):
        return dot(a, b).astype(BF16).astype(F32)

    def pass_on(i):
        att_copy(i).wait_recv()
        summed = rounded(att[i, 0], wout[:, theirs]) + rounded(att[i, 1], wo[1])
        part_s[i] = summed.astype(BF16)
        part_copy(i).start()

    def finish(i):
        proj = rounded(att[i, 0], wout[:, own]) + rounded(att[i, 1], wo[0])
        part_copy(i).wait_recv()
        proj = proj + part_r[i].astype(F32)
        lay[tok * i : tok * (i + 1), :] = (lat[i, :, own].astype(F32) + proj).astype(BF16)

    n_slots = nv * cap

    def select_mine():
        places = jnp.transpose(idxs[...])
        for c in range(mb.shape[0]):
            at = places[:, c : c + 1].astype(I32)
            hit = at == lax.broadcasted_iota(I32, (lanes, n_slots), 1)
            fsel[lanes * c : lanes * (c + 1), :] = hit.astype(F32).astype(BF16)

    def select_asked():
        for o in range(nv - 1):
            req_copy(o).wait()
        asked = jnp.transpose(reqi[:, 0, :])
        for k in range(nv):
            hit = asked[:cap, k : k + 1] == lax.broadcasted_iota(I32, (cap, nl * tok), 1)
            gsel[cap * k : cap * (k + 1), :] = hit.astype(F32).astype(BF16)

    for n, i in enumerate(ORDER):
        with scope(f"halo{n}"):
            kv_copy((3, 0, 2, 1)[n]).wait_recv()
        with scope(f"att{n}"):
            attend(i)
        att_copy(i).start()
        if n == 1:
            for k in (0, 1):
                wo_copy(k).wait()
        if n > 1:
            with scope(f"pass{n}"):
                pass_on(ORDER[n - 2])

    with scope("sel_mine"):
        select_mine()
    with scope("pass4"):
        pass_on(ORDER[2])
    with scope("sel_asked"):
        select_asked()
    with scope("pass5"):
        pass_on(ORDER[3])
    for n, i in enumerate(ORDER):
        with scope(f"finish{n}"):
            finish(i)
    lay_copy = pltpu.make_async_copy(lay, lay_out, out_sem.at[0])
    lay_copy.start()

    for lo, hi in PICK_GROUPS:
        with scope(f"pick{lo}"):
            picked = dot(gsel[cap * lo : cap * hi, :], lay[...]).astype(BF16)
            picked = picked.reshape(hi - lo, cap, sub)
            rows[lo:hi] = picked
            if hi == nv:
                reps[nv - 1] = picked[-1]
            for o in range(lo, min(hi, nv - 1)):
                rep_copy(o).start()

    for lo, hi in TAKE_GROUPS:
        with scope(f"take{lo}"):
            for o in range(lo, min(hi, nv - 1)):
                rep_copy(o).wait()
            block = reps[lo:hi].reshape((hi - lo) * cap, sub)
            part = dot(fsel[:, cap * lo : cap * hi], block)
            if lo > 0:
                part = acc[...] + part
            if hi < nv:
                acc[...] = part
            else:
                got[...] = part.astype(BF16)
    got_copy = pltpu.make_async_copy(got, got_out, out_sem.at[1])
    got_copy.start()

    for i in range(nl):
        kv_copy(i).wait_send()
        att_copy(i).wait_send()
        part_copy(i).wait_send()
    lay_copy.wait()
    got_copy.wait()


def per_device(nv, latents, norm_gain, w_qkv, w_out, intersection, match_block, match_row, confidence):
    nl, tok, width = latents.shape
    sub = w_qkv.shape[2]
    rows = nl * tok
    cap = 2 * rows // nv
    here = pl.BlockSpec(memory_space=pl.ANY)
    dma = pltpu.SemaphoreType.DMA
    vmem = pltpu.VMEM
    lanes = 128
    lay, got = pl.pallas_call(
        functools.partial(kernel, nv, nl * nv, cap),
        out_shape=[jax.ShapeDtypeStruct((rows, sub), BF16)] * 2,
        in_specs=[here] * 7,
        out_specs=[here] * 2,
        scratch_shapes=[
            vmem((nl, tok, width), BF16),
            vmem((1, width), F32),
            vmem((3, width, sub), BF16),
            vmem((sub, width), BF16),
            pltpu.SMEM(intersection.shape[::-1], I32),
            vmem((rows // lanes, lanes), I32),
            vmem((rows // lanes, lanes), I32),
            vmem((nl + 4, tok, 2 * sub), BF16),
            vmem((nl, tok, sub), BF16),
            vmem((nl, 2, tok, sub), BF16),
            vmem((2, sub, sub), BF16),
            vmem((nl, tok, sub), BF16),
            vmem((nl, tok, sub), BF16),
            vmem((rows, sub), BF16),
            vmem((nv * cap, rows), BF16),
            vmem((rows, nv * cap), BF16),
            vmem((rows // lanes, lanes), F32),
            vmem((nv, 8, lanes), I32),
            vmem((nv, 8, lanes), I32),
            vmem((nv, cap, sub), BF16),
            vmem((nv, cap, sub), BF16),
            vmem((rows, sub), F32),
            vmem((rows, sub), BF16),
            dma((12,)), dma((2,)),
            dma((nl,)), dma((nl,)), dma((2,)), dma((2,)),
            dma((nl,)), dma((nl,)), dma((nl,)), dma((nl,)),
            dma((nv,)), dma((nv,)), dma((nv,)), dma((nv,)),
        ],
        compiler_params=pltpu.CompilerParams(
            collective_id=0, has_side_effects=True, vmem_limit_bytes=60 * 1024 * 1024
        ),
    )(
        latents,
        norm_gain.reshape(1, width),
        w_qkv,
        w_out,
        intersection.T,
        match_block.reshape(rows // lanes, lanes),
        match_row.reshape(rows // lanes, lanes),
    )
    mine = lay.astype(F32)
    refined = mine + COUPLING * confidence[:, None] * (got.astype(F32) - mine)
    return refined.reshape(nl, tok, sub)


def solution(mesh):
    in_specs = (
        P("views", None, None),
        P(),
        P(None, None, "heads"),
        P("heads", None),
        P(),
        P("views", None),
        P("views"),
        P("views"),
    )
    out_specs = P("views", None, "heads")
    return jax.shard_map(
        functools.partial(per_device, mesh.shape["views"]),
        mesh=mesh, in_specs=in_specs, out_specs=out_specs, check_vma=False,
    )
```

```python
import functools

import jax
import jax.numpy as jnp
from jax import lax
from jax.experimental import pallas as pl
from jax.experimental.pallas import tpu as pltpu
from jax.sharding import PartitionSpec as P

MESH = pl.DeviceIdType.MESH
F32, BF16, I32 = jnp.float32, jnp.bfloat16, jnp.int32
EPSILON = 1e-06
COUPLING = 0.5
HEAD_DIM = 64
ORDER = (1, 0, 2, 3)
SIDE = 4
VMEM_MIB = 60


def ring_steps(d):
    return min(d, SIDE - d)


PLACES = sorted(
    ((dx, dy, dc) for dx in range(SIDE) for dy in range(SIDE) for dc in range(2)),
    key=lambda p: (-ring_steps(p[0]) - ring_steps(p[1]), -p[2]),
)
PICK_GROUPS = ((0, 4), (4, 8), (8, 16), (16, 24), (24, 32))
TAKE_GROUPS = ((0, 8), (8, 16), (16, 24), (24, 32))


def dot(a, b):
    return jnp.dot(a, b, preferred_element_type=F32)


def dot_nt(a, b):
    return lax.dot_general(a, b, (((1,), (1,)), ((), ())), preferred_element_type=F32)


def scope(name):
    return jax.named_scope(name)


def kernel(
    nv, views_total, cap,
    lat_h, gain_h, wqkv_h, wout_h, inter_h, mb_h, mr_h,
    lay_out, got_out,
    lat, gain, wqkv, wout, inter, mb, mr,
    kv, q, att, wo, part_s, part_r, lay, gsel, fsel, idxs, reqo, reqi, rows, reps, acc, normed,
    in_sem, kv_s, kv_r, wo_s, wo_r, at_s, at_r, pt_s, pt_r, rq_s, rq_r, rp_s, rp_r,
):
    nl, tok, width = lat.shape
    sub = wqkv.shape[2]
    me = lax.axis_index("views")
    z = lax.axis_index("heads")
    odd = lax.rem(z, 2)
    pair, opp = z + 1 - 2 * odd, lax.rem(z + 3 + 2 * odd, 4)
    far = lax.rem(z + 2, 4)
    px, py, pc = me // (2 * SIDE), lax.rem(me // 2, SIDE), lax.rem(me, 2)
    partner = me + 1 - 2 * pc
    beyond = lax.rem(me + nv - 1 + 2 * pc, nv)

    def actual(u):
        return u * pc + (nl - 1 - u) * (1 - pc)

    def away(o, sign):
        dx, dy, dc = PLACES[o]
        bx = lax.rem(px + (dx if sign > 0 else SIDE - dx), SIDE)
        by = lax.rem(py + (dy if sign > 0 else SIDE - dy), SIDE)
        return bx * (2 * SIDE) + by * 2 + lax.rem(pc + dc, 2)

    def load(n, src, dst):
        copy = pltpu.make_async_copy(src, dst, in_sem.at[n])
        copy.start()
        return copy

    in_gain = load(0, gain_h, gain)
    in_lat = {3: load(1, lat_h.at[actual(3)], lat.at[3])}
    in_k = load(2, wqkv_h.at[1], wqkv.at[1])
    in_v = load(3, wqkv_h.at[2], wqkv.at[2])
    for u in (2, 0, 1):
        in_lat[u] = load(6 + u, lat_h.at[actual(u)], lat.at[u])
    in_wout = load(5, wout_h, wout)
    in_q = load(4, wqkv_h.at[0], wqkv.at[0])
    in_small = [load(9, mb_h, mb), load(10, mr_h, mr), load(11, inter_h, inter)]

    def remote(src, dst, send, recv, device):
        return pltpu.make_async_remote_copy(
            src_ref=src, dst_ref=dst, send_sem=send, recv_sem=recv,
            device_id=device, device_id_type=MESH,
        )

    barrier = pltpu.get_barrier_semaphore()

    def greet(k, carry):
        pl.semaphore_signal(
            barrier, inc=1, device_id=(lax.rem(me + k, nv), z), device_id_type=MESH
        )
        return carry

    lax.fori_loop(1, nv, greet, 0)
    for other in (pair, opp):
        pl.semaphore_signal(barrier, inc=1, device_id=(me, other), device_id_type=MESH)

    def kv_copy(u):
        slot = (1, 0, nl + 3, nl + 2)[u]
        target = partner if u < 2 else beyond
        return remote(kv.at[2 + u], kv.at[slot], kv_s.at[u], kv_r.at[u], (target, z))

    def wo_copy(n):
        cols = pl.ds(pl.multiple_of((pair, far, opp, far)[n] * sub, sub), sub)
        target = (pair, opp)[n // 2]
        return remote(wout.at[:, cols], wo.at[n], wo_s.at[n], wo_r.at[n], (me, target))

    def ways(n):
        return (pair, opp) if n % 2 == 0 else (opp, pair)

    def att_copy(n):
        return remote(att.at[n, 0], att.at[n, 1], at_s.at[n], at_r.at[n], (me, ways(n)[0]))

    def part_copy(n):
        return remote(part_s.at[n], part_r.at[n], pt_s.at[n], pt_r.at[n], (me, ways(n)[1]))

    def req_copy(o):
        return remote(reqo.at[o], reqi.at[o], rq_s.at[o], rq_r.at[o], (away(o, 1), z))

    def rep_copy(o):
        return remote(rows.at[o], reps.at[o], rp_s.at[o], rp_r.at[o], (away(o, -1), z))

    in_gain.wait()
    for n, u in enumerate((3, 2, 0, 1)):
        with scope(f"proj{n}"):
            in_lat[u].wait()
            wide = lat[u].astype(F32)
            mean_square = jnp.mean(wide * wide, axis=-1, keepdims=True)
            x = (wide * lax.rsqrt(mean_square + EPSILON) * gain[...]).astype(BF16)
            normed[u] = x
            if n == 0:
                in_k.wait()
            kv[2 + u, :, :sub] = dot(x, wqkv[1]).astype(BF16)
            if n == 0:
                in_v.wait()
            kv[2 + u, :, sub:] = dot(x, wqkv[2]).astype(BF16)
        if n == 2:
            with scope("greeted"):
                pl.semaphore_wait(barrier, nv + 1)
            for early in (0, 3, 2):
                kv_copy(early).start()
            in_wout.wait()
            for k in range(4):
                wo_copy(k).start()
    kv_copy(1).start()
    in_q.wait()
    for copy in in_small:
        copy.wait()

    def ask(u):
        found = dot(normed[u], wqkv[0]).astype(BF16).astype(F32)
        q[u] = (found * HEAD_DIM ** (-0.5)).astype(BF16)

    lanes = mb.shape[1]

    def prepare():
        named = mb[...]
        rel = (((named >> 3) - px) & 3) * 8 + ((((named >> 1) & 3) - py) & 3) * 2 + ((named - pc) & 1)
        place = jnp.zeros_like(rel)
        for o, (dx, dy, dc) in enumerate(PLACES):
            place = jnp.where(rel == dx * 8 + dy * 2 + dc, o, place)
        wanted = mr[...]
        block_iota = lax.broadcasted_iota(I32, (nv, lanes), 0)
        slot_iota = lax.broadcasted_iota(I32, (lanes, lanes), 0)
        before = (slot_iota < lax.broadcasted_iota(I32, (lanes, lanes), 1)).astype(F32).astype(BF16)
        base = jnp.zeros((nv, 1), F32)
        digits = jnp.zeros((2 * nv, lanes), F32)
        for c in range(mb.shape[0]):
            onehot = (place[c : c + 1] == block_iota).astype(F32)
            earlier = dot(onehot.astype(BF16), before) + base
            slot = jnp.sum(onehot * earlier, axis=0, keepdims=True)
            base = base + jnp.sum(onehot, axis=1, keepdims=True)
            idxs[c : c + 1, :] = place[c : c + 1].astype(F32) * cap + slot
            is_slot = (slot.astype(I32) == slot_iota).astype(F32).astype(BF16)
            row = wanted[c : c + 1]
            high, low = (row >> 5).astype(F32), (row & 31).astype(F32)
            both = jnp.concatenate([onehot * high, onehot * low], axis=0).astype(BF16)
            digits = digits + dot_nt(both, is_slot)
        requests = (digits[:nv] * 32.0 + digits[nv:]).astype(I32)
        for k in range(nv):
            reqo[k] = jnp.broadcast_to(requests[k : k + 1], reqo.shape[1:])
        reqi[nv - 1] = jnp.broadcast_to(requests[nv - 1 : nv], reqo.shape[1:])
        for o in range(nv - 1):
            req_copy(o).start()

    lane = lax.broadcasted_iota(I32, (1, 2 * HEAD_DIM), 1)
    first = lane < HEAD_DIM

    def attend(n, i):
        a = me * nl + actual(i)
        bias = []
        for j in range(5):
            d = j - 2
            if d == 0:
                bias.append(None)
            else:
                back = d * (1 - pc) if d > 0 else -d * pc
                source = lax.rem(a - back + views_total, views_total)
                present = inter[abs(d) - 1, source]
                bias.append((present.astype(F32) - 1.0) * 1e30)
        for t in range(sub // (2 * HEAD_DIM)):
            k_cols = slice(2 * HEAD_DIM * t, 2 * HEAD_DIM * (t + 1))
            v_cols = slice(sub + 2 * HEAD_DIM * t, sub + 2 * HEAD_DIM * (t + 1))
            both = q[i, :, k_cols]
            done = []
            for mine in (first, jnp.logical_not(first)):
                query = jnp.where(mine, both, jnp.zeros_like(both))
                scores = []
                for j in range(5):
                    s = dot_nt(query, kv[i + j, :, k_cols])
                    scores.append(s if bias[j] is None else s + bias[j])
                top = functools.reduce(jnp.maximum, scores)
                top = jnp.max(top, axis=-1, keepdims=True)
                numer, total = None, None
                for j in range(5):
                    p = jnp.exp(scores[j] - top)
                    total = p if total is None else total + p
                    part = dot(p.astype(BF16), kv[i + j, :, v_cols])
                    numer = part if numer is None else numer + part
                total = jnp.sum(total, axis=-1, keepdims=True)
                done.append(numer / total)
            att[n, 0, :, k_cols] = jnp.where(first, done[0], done[1]).astype(BF16)

    own, to_pair, to_opp = (
        pl.ds(pl.multiple_of(g * sub, sub), sub) for g in (z, pair, opp)
    )

    def rounded(a, b):
        return dot(a, b).astype(BF16).astype(F32)

    def pass_on(n):
        att_copy(n).wait_recv()
        cols, block = ((to_opp, 1), (to_pair, 3))[n % 2]
        summed = rounded(att[n, 0], wout[:, cols]) + rounded(att[n, 1], wo[block])
        part_s[n] = summed.astype(BF16)
        part_copy(n).start()

    def finish(n):
        u = ORDER[n]
        proj = rounded(att[n, 0], wout[:, own]) + rounded(att[n, 1], wo[2 * (n % 2)])
        part_copy(n).wait_recv()
        proj = proj + part_r[n].astype(F32)
        done = (lat[u, :, own].astype(F32) + proj).astype(BF16)
        lay[pl.ds(pl.multiple_of(actual(u) * tok, tok), tok), :] = done

    n_slots = nv * cap

    def select_mine():
        places = jnp.transpose(idxs[...])
        for c in range(mb.shape[0]):
            at = places[:, c : c + 1].astype(I32)
            hit = at == lax.broadcasted_iota(I32, (lanes, n_slots), 1)
            fsel[lanes * c : lanes * (c + 1), :] = hit.astype(F32).astype(BF16)

    def select_asked():
        for o in range(nv - 1):
            req_copy(o).wait()
        asked = jnp.transpose(reqi[:, 0, :])
        for k in range(nv):
            hit = asked[:cap, k : k + 1] == lax.broadcasted_iota(I32, (cap, nl * tok), 1)
            gsel[cap * k : cap * (k + 1), :] = hit.astype(F32).astype(BF16)

    for n, u in enumerate(ORDER):
        with scope(f"ask{n}"):
            ask(u)
        with scope(f"halo{n}"):
            kv_copy((0, 1, 3, 2)[n]).wait_recv()
        with scope(f"att{n}"):
            attend(n, u)
        att_copy(n).start()
        if n == 0:
            with scope("prep"):
                prepare()
        if n == 1:
            for k in range(4):
                wo_copy(k).wait()
        if n > 1:
            with scope(f"pass{n}"):
                pass_on(n - 2)

    with scope("sel_mine"):
        select_mine()
    with scope("pass4"):
        pass_on(2)
    with scope("sel_asked"):
        select_asked()
    with scope("pass5"):
        pass_on(3)
    for n in range(nl):
        with scope(f"finish{n}"):
            finish(n)
            lay_out[pl.ds(pl.multiple_of(actual(ORDER[n]) * tok, tok), tok), :] = lay[
                pl.ds(pl.multiple_of(actual(ORDER[n]) * tok, tok), tok), :
            ]

    for lo, hi in PICK_GROUPS:
        with scope(f"pick{lo}"):
            picked = dot(gsel[cap * lo : cap * hi, :], lay[...]).astype(BF16)
            picked = picked.reshape(hi - lo, cap, sub)
            rows[lo:hi] = picked
            if hi == nv:
                reps[nv - 1] = picked[-1]
            for o in range(lo, min(hi, nv - 1)):
                rep_copy(o).start()

    for lo, hi in TAKE_GROUPS:
        with scope(f"take{lo}"):
            for o in range(lo, min(hi, nv - 1)):
                rep_copy(o).wait()
            block = reps[lo:hi].reshape((hi - lo) * cap, sub)
            part = dot(fsel[:, cap * lo : cap * hi], block)
            if lo > 0:
                part = acc[...] + part
            if hi < nv:
                acc[...] = part
            else:
                got_out[...] = part.astype(BF16)

    for i in range(nl):
        kv_copy(i).wait_send()
        att_copy(i).wait_send()
        part_copy(i).wait_send()


def per_device(nv, latents, norm_gain, w_qkv, w_out, intersection, match_block, match_row, confidence):
    nl, tok, width = latents.shape
    sub = w_qkv.shape[2]
    rows = nl * tok
    cap = 2 * rows // nv
    here = pl.BlockSpec(memory_space=pltpu.HBM)
    dma = pltpu.SemaphoreType.DMA
    vmem = pltpu.VMEM
    lanes = 128
    lay, got = pl.pallas_call(
        functools.partial(kernel, nv, nl * nv, cap),
        out_shape=[jax.ShapeDtypeStruct((rows, sub), BF16)] * 2,
        in_specs=[here] * 7,
        out_specs=[pl.BlockSpec(memory_space=pltpu.VMEM)] * 2,
        scratch_shapes=[
            vmem((nl, tok, width), BF16),
            vmem((1, width), F32),
            vmem((3, width, sub), BF16),
            vmem((sub, width), BF16),
            pltpu.SMEM(intersection.shape[::-1], I32),
            vmem((rows // lanes, lanes), I32),
            vmem((rows // lanes, lanes), I32),
            vmem((nl + 4, tok, 2 * sub), BF16),
            vmem((nl, tok, sub), BF16),
            vmem((nl, 2, tok, sub), BF16),
            vmem((4, sub, sub), BF16),
            vmem((nl, tok, sub), BF16),
            vmem((nl, tok, sub), BF16),
            vmem((rows, sub), BF16),
            vmem((nv * cap, rows), BF16),
            vmem((rows, nv * cap), BF16),
            vmem((rows // lanes, lanes), F32),
            vmem((nv, 8, lanes), I32),
            vmem((nv, 8, lanes), I32),
            vmem((nv, cap, sub), BF16),
            vmem((nv, cap, sub), BF16),
            vmem((rows, sub), F32),
            vmem((nl, tok, width), BF16),
            dma((12,)),
            dma((nl,)), dma((nl,)), dma((4,)), dma((4,)),
            dma((nl,)), dma((nl,)), dma((nl,)), dma((nl,)),
            dma((nv,)), dma((nv,)), dma((nv,)), dma((nv,)),
        ],
        compiler_params=pltpu.CompilerParams(
            collective_id=0, has_side_effects=True, vmem_limit_bytes=VMEM_MIB * 1024 * 1024
        ),
    )(
        latents,
        norm_gain.reshape(1, width),
        w_qkv,
        w_out,
        intersection.T,
        match_block.reshape(rows // lanes, lanes),
        match_row.reshape(rows // lanes, lanes),
    )
    mine = lay.astype(F32)
    refined = mine + COUPLING * (confidence[:, None] * (got.astype(F32) - mine))
    return refined.reshape(nl, tok, sub)


def solution(mesh):
    in_specs = (
        P("views", None, None),
        P(),
        P(None, None, "heads"),
        P("heads", None),
        P(),
        P("views", None),
        P("views"),
        P("views"),
    )
    out_specs = P("views", None, "heads")
    return jax.shard_map(
        functools.partial(per_device, mesh.shape["views"]),
        mesh=mesh, in_specs=in_specs, out_specs=out_specs, check_vma=False,
    )
```

```python
import functools

import jax
import jax.numpy as jnp
from jax import lax
from jax.experimental import pallas as pl
from jax.experimental.pallas import tpu as pltpu
from jax.sharding import PartitionSpec as P

MESH = pl.DeviceIdType.MESH
F32, BF16, I32 = jnp.float32, jnp.bfloat16, jnp.int32
EPSILON = 1e-06
COUPLING = 0.5
LOG2_E = 1.4426950408889634
HEAD_DIM = 64
ORDER = (1, 0, 2, 3)
SIDE = 4
VMEM_MIB = 60


def ring_steps(d):
    return min(d, SIDE - d)


PLACES = sorted(
    ((dx, dy, dc) for dx in range(SIDE) for dy in range(SIDE) for dc in range(2)),
    key=lambda p: (-ring_steps(p[0]) - ring_steps(p[1]), -p[2]),
)
PICK_GROUPS = ((0, 4), (4, 8), (8, 16), (16, 24), (24, 32))
TAKE_GROUPS = ((0, 8), (8, 16), (16, 24), (24, 28), (28, 32))


def dot(a, b):
    return jnp.dot(a, b, preferred_element_type=F32)


def dot_nt(a, b):
    return lax.dot_general(a, b, (((1,), (1,)), ((), ())), preferred_element_type=F32)


def value_rows(h):
    start = 256 + (2 * HEAD_DIM + 16) * (h // 2) + (h % 2) * HEAD_DIM
    return start, start + 16 * (h % 2)


def scope(name):
    return jax.named_scope(name)


def kernel(
    nv, views_total, cap,
    lat_h, gain_h, wqkv_h, wout_h, inter_h, mb_h, mr_h,
    lay_out, got_out,
    lat, gain, wqkv, wout, inter, mb, mr,
    kv, q, att, wo, part_s, part_r, lay, gsel, fsel, idxs, reqo, reqi, rows, reps, acc, normed, turned,
    in_sem, kv_s, kv_r, wo_s, wo_r, ws_s, ws_r, at_s, at_r, pt_s, pt_r, rq_s, rq_r, rp_s, rp_r,
):
    nl, tok, width = lat.shape
    sub = wqkv.shape[2]
    me = lax.axis_index("views")
    z = lax.axis_index("heads")
    odd = lax.rem(z, 2)
    pair, opp = z + 1 - 2 * odd, lax.rem(z + 3 + 2 * odd, 4)
    far = lax.rem(z + 2, 4)
    px, py, pc = me // (2 * SIDE), lax.rem(me // 2, SIDE), lax.rem(me, 2)
    partner = me + 1 - 2 * pc
    beyond = lax.rem(me + nv - 1 + 2 * pc, nv)

    def actual(u):
        return u * pc + (nl - 1 - u) * (1 - pc)

    def away(o, sign):
        dx, dy, dc = PLACES[o]
        bx = lax.rem(px + (dx if sign > 0 else SIDE - dx), SIDE)
        by = lax.rem(py + (dy if sign > 0 else SIDE - dy), SIDE)
        return bx * (2 * SIDE) + by * 2 + lax.rem(pc + dc, 2)

    def load(n, src, dst):
        copy = pltpu.make_async_copy(src, dst, in_sem.at[n])
        copy.start()
        return copy

    in_gain = load(0, gain_h, gain)
    in_lat = {3: load(1, lat_h.at[actual(3)], lat.at[3])}
    in_k = load(2, wqkv_h.at[1], wqkv.at[1])
    in_v = load(3, wqkv_h.at[2], wqkv.at[2])
    for u in (2, 0, 1):
        in_lat[u] = load(6 + u, lat_h.at[actual(u)], lat.at[u])
    in_wout = load(5, wout_h, wout)
    in_q = load(4, wqkv_h.at[0], wqkv.at[0])
    in_small = [load(9, mb_h, mb), load(10, mr_h, mr), load(11, inter_h, inter)]

    def remote(src, dst, send, recv, device):
        return pltpu.make_async_remote_copy(
            src_ref=src, dst_ref=dst, send_sem=send, recv_sem=recv,
            device_id=device, device_id_type=MESH,
        )

    barrier = pltpu.get_barrier_semaphore()

    def greet(k, carry):
        pl.semaphore_signal(
            barrier, inc=1, device_id=(lax.rem(me + k, nv), z), device_id_type=MESH
        )
        return carry

    lax.fori_loop(1, nv, greet, 0)
    for other in (pair, opp):
        pl.semaphore_signal(barrier, inc=1, device_id=(me, other), device_id_type=MESH)

    def kv_copy(u):
        slot = (1, 0, nl + 3, nl + 2)[u]
        target = partner if u < 2 else beyond
        return remote(kv.at[2 + u], kv.at[slot], kv_s.at[u], kv_r.at[u], (target, z))

    half = sub // 2
    my_half = pl.ds(pl.multiple_of(pc * half, half), half)

    def wo_copy(n):
        cols = pl.ds(pl.multiple_of((pair, far, opp, far)[n] * sub, sub), sub)
        target = (pair, opp)[n // 2]
        return remote(
            wout.at[my_half, cols], wo.at[n, my_half], wo_s.at[n], wo_r.at[n], (me, target)
        )

    def wo_share(n):
        block = wo.at[n, my_half]
        return remote(block, block, ws_s.at[n], ws_r.at[n], (partner, z))

    def ways(n):
        return (pair, opp) if n % 2 == 0 else (opp, pair)

    def pieces(n):
        size = tok // 2 if n == nl - 1 else tok
        return [(c, pl.ds(c * size, size)) for c in range(tok // size)]

    def att_copy(n, c, part):
        return remote(
            att.at[n, 0, part], att.at[n, 1, part], at_s.at[n, c], at_r.at[n, c], (me, ways(n)[0])
        )

    def part_copy(n, c, part):
        return remote(
            part_s.at[n, part], part_r.at[n, part], pt_s.at[n, c], pt_r.at[n, c], (me, ways(n)[1])
        )

    def req_copy(o):
        return remote(reqo.at[o], reqi.at[o], rq_s.at[o], rq_r.at[o], (away(o, 1), z))

    def rep_copy(o):
        return remote(rows.at[o], reps.at[o], rp_s.at[o], rp_r.at[o], (away(o, -1), z))

    in_gain.wait()
    for n, u in enumerate((3, 2, 0, 1)):
        with scope(f"proj{n}"):
            in_lat[u].wait()
            wide = lat[u].astype(F32)
            mean_square = jnp.mean(wide * wide, axis=-1, keepdims=True)
            x = (wide * lax.rsqrt(mean_square + EPSILON) * gain[...]).astype(BF16)
            normed[u] = x
            if n == 0:
                in_k.wait()
            kv[2 + u, :tok, :] = dot(x, wqkv[1]).astype(BF16)
            if n == 0:
                in_v.wait()
            values = jnp.transpose(dot(x, wqkv[2])).astype(BF16)
            for h in range(sub // HEAD_DIM):
                top, first_row = value_rows(h)
                kv[2 + u, first_row : first_row + HEAD_DIM, :] = values[HEAD_DIM * h : HEAD_DIM * (h + 1)]
                if h % 2 == 0:
                    kv[2 + u, first_row + HEAD_DIM : first_row + HEAD_DIM + 16, :] = jnp.ones((16, tok), BF16)
        if n == 2:
            with scope("greeted"):
                pl.semaphore_wait(barrier, nv + 1)
            for early in (0, 3, 2):
                kv_copy(early).start()
            in_wout.wait()
            for k in range(4):
                wo_copy(k).start()
    kv_copy(1).start()
    in_q.wait()
    for copy in in_small:
        copy.wait()

    def ask(begin, end):
        found = dot(normed[begin:end].reshape((end - begin) * tok, width), wqkv[0])
        found = (found * (HEAD_DIM ** (-0.5) * LOG2_E)).astype(BF16)
        q[begin:end] = found.reshape(end - begin, tok, sub)

    lanes = mb.shape[1]

    def prepare():
        named = mb[...]
        rel = (((named >> 3) - px) & 3) * 8 + ((((named >> 1) & 3) - py) & 3) * 2 + ((named - pc) & 1)
        place = jnp.zeros_like(rel)
        for o, (dx, dy, dc) in enumerate(PLACES):
            place = jnp.where(rel == dx * 8 + dy * 2 + dc, o, place)
        wanted = mr[...]
        block_iota = lax.broadcasted_iota(I32, (nv, lanes), 0)
        slot_iota = lax.broadcasted_iota(I32, (lanes, lanes), 0)
        before = (slot_iota < lax.broadcasted_iota(I32, (lanes, lanes), 1)).astype(F32).astype(BF16)
        base = jnp.zeros((nv, 1), F32)
        digits = jnp.zeros((2 * nv, lanes), F32)
        for c in range(mb.shape[0]):
            onehot = (place[c : c + 1] == block_iota).astype(F32)
            earlier = dot(onehot.astype(BF16), before) + base
            slot = jnp.sum(onehot * earlier, axis=0, keepdims=True)
            base = base + jnp.sum(onehot, axis=1, keepdims=True)
            idxs[c : c + 1, :] = place[c : c + 1].astype(F32) * cap + slot
            is_slot = (slot.astype(I32) == slot_iota).astype(F32).astype(BF16)
            row = wanted[c : c + 1]
            high, low = (row >> 5).astype(F32), (row & 31).astype(F32)
            both = jnp.concatenate([onehot * high, onehot * low], axis=0).astype(BF16)
            digits = digits + dot_nt(both, is_slot)
        requests = (digits[:nv] * 32.0 + digits[nv:]).astype(I32)
        for k in range(nv):
            reqo[k] = jnp.broadcast_to(requests[k : k + 1], reqo.shape[1:])
        reqi[nv - 1] = jnp.broadcast_to(requests[nv - 1 : nv], reqo.shape[1:])
        for o in range(nv - 1):
            req_copy(o).start()

    lane = lax.broadcasted_iota(I32, (1, 2 * HEAD_DIM), 1)
    first = lane < HEAD_DIM

    def attend(n, i):
        a = me * nl + actual(i)
        bias = []
        for j in range(5):
            d = j - 2
            if d == 0:
                bias.append(None)
            else:
                back = d * (1 - pc) if d > 0 else -d * pc
                source = lax.rem(a - back + views_total, views_total)
                present = inter[abs(d) - 1, source]
                bias.append((1.0 - present.astype(F32)) * 1e30)
        heads = sub // HEAD_DIM
        scores = []
        for h in range(heads):
            cols = slice(2 * HEAD_DIM * (h // 2), 2 * HEAD_DIM * (h // 2 + 1))
            both = q[i, :, cols]
            mine = first if h % 2 == 0 else jnp.logical_not(first)
            query = jnp.where(mine, both, jnp.zeros_like(both))
            tiles = []
            for j in range(5):
                s = dot_nt(kv[i + j, :tok, cols], query)
                high = jnp.max(s.reshape(tok // 8, 8, tok), axis=0)
                tiles.append((s, high if bias[j] is None else high - bias[j]))
            scores.append(tiles)
        for h in range(heads):
            top = functools.reduce(jnp.maximum, [high for _, high in scores[h]])
            top = jnp.max(top, axis=0, keepdims=True)
            found = None
            begin, _ = value_rows(h)
            for j in range(5):
                p = jnp.exp2(scores[h][j][0] - (top if bias[j] is None else top + bias[j]))
                part = dot(kv[i + j, begin : begin + HEAD_DIM + 16, :], p.astype(BF16))
                found = part if found is None else found + part
            if h % 2 == 0:
                numer, total = found[:HEAD_DIM], found[HEAD_DIM : HEAD_DIM + 1]
            else:
                numer, total = found[16:], found[0:1]
            turned[HEAD_DIM * h : HEAD_DIM * (h + 1), :] = numer / total
        att[n, 0] = jnp.transpose(turned[...]).astype(BF16)

    own, to_pair, to_opp = (
        pl.ds(pl.multiple_of(g * sub, sub), sub) for g in (z, pair, opp)
    )

    def rounded(a, b):
        return dot(a, b).astype(BF16).astype(F32)

    def pass_on(n):
        cols, block = ((to_opp, 1), (to_pair, 3))[n % 2]
        for c, part in pieces(n):
            att_copy(n, c, part).wait_recv()
            summed = rounded(att[n, 0, part], wout[:, cols]) + rounded(att[n, 1, part], wo[block])
            part_s[n, part] = summed.astype(BF16)
            part_copy(n, c, part).start()

    def finish(n):
        u = ORDER[n]
        proj = rounded(att[n, 0], wout[:, own]) + rounded(att[n, 1], wo[2 * (n % 2)])
        for c, part in pieces(n):
            part_copy(n, c, part).wait_recv()
        proj = proj + part_r[n].astype(F32)
        done = (lat[u, :, own].astype(F32) + proj).astype(BF16)
        lay[pl.ds(pl.multiple_of(actual(u) * tok, tok), tok), :] = done

    n_slots = nv * cap

    def select_mine():
        places = jnp.transpose(idxs[...])
        for c in range(mb.shape[0]):
            at = places[:, c : c + 1].astype(I32)
            hit = at == lax.broadcasted_iota(I32, (lanes, n_slots), 1)
            fsel[lanes * c : lanes * (c + 1), :] = hit.astype(F32).astype(BF16)

    def select_asked():
        for o in range(nv - 1):
            req_copy(o).wait()
        asked = jnp.transpose(reqi[:, 0, :])
        for k in range(nv):
            hit = asked[:cap, k : k + 1] == lax.broadcasted_iota(I32, (cap, nl * tok), 1)
            gsel[cap * k : cap * (k + 1), :] = hit.astype(F32).astype(BF16)

    for n, u in enumerate(ORDER):
        with scope(f"halo{n}"):
            kv_copy((0, 1, 3, 2)[n]).wait_recv()
        with scope(f"att{n}"):
            if n == 0:
                ask(0, nl)
            attend(n, u)
        for c, part in pieces(n):
            att_copy(n, c, part).start()
        if n == 1:
            for k in range(4):
                wo_copy(k).wait()
                wo_share(k).start()
        if n == 2:
            with scope("wo"):
                for k in range(4):
                    wo_share(k).wait()
        if n > 1:
            with scope(f"pass{n}"):
                pass_on(n - 2)

    with scope("prep"):
        prepare()
    with scope("sel_mine"):
        select_mine()
    with scope("pass4"):
        pass_on(2)
    with scope("pass5"):
        pass_on(3)
    with scope("sel_asked"):
        select_asked()
    for n in range(nl):
        with scope(f"finish{n}"):
            finish(n)
            lay_out[pl.ds(pl.multiple_of(actual(ORDER[n]) * tok, tok), tok), :] = lay[
                pl.ds(pl.multiple_of(actual(ORDER[n]) * tok, tok), tok), :
            ]

    for lo, hi in PICK_GROUPS:
        with scope(f"pick{lo}"):
            picked = dot(gsel[cap * lo : cap * hi, :], lay[...]).astype(BF16)
            picked = picked.reshape(hi - lo, cap, sub)
            rows[lo:hi] = picked
            if hi == nv:
                reps[nv - 1] = picked[-1]
            for o in range(lo, min(hi, nv - 1)):
                rep_copy(o).start()

    for lo, hi in TAKE_GROUPS:
        with scope(f"take{lo}"):
            for o in range(lo, min(hi, nv - 1)):
                rep_copy(o).wait()
            block = reps[lo:hi].reshape((hi - lo) * cap, sub)
            part = dot(fsel[:, cap * lo : cap * hi], block)
            if lo > 0:
                part = acc[...] + part
            if hi < nv:
                acc[...] = part
            else:
                got_out[...] = part.astype(BF16)

    for i in range(nl):
        kv_copy(i).wait_send()
        for c, part in pieces(i):
            att_copy(i, c, part).wait_send()
            part_copy(i, c, part).wait_send()


def per_device(nv, latents, norm_gain, w_qkv, w_out, intersection, match_block, match_row, confidence):
    nl, tok, width = latents.shape
    sub = w_qkv.shape[2]
    rows = nl * tok
    cap = 2 * rows // nv
    here = pl.BlockSpec(memory_space=pltpu.HBM)
    dma = pltpu.SemaphoreType.DMA
    vmem = pltpu.VMEM
    lanes = 128
    lay, got = pl.pallas_call(
        functools.partial(kernel, nv, nl * nv, cap),
        out_shape=[jax.ShapeDtypeStruct((rows, sub), BF16)] * 2,
        in_specs=[here] * 7,
        out_specs=[pl.BlockSpec(memory_space=pltpu.VMEM)] * 2,
        scratch_shapes=[
            vmem((nl, tok, width), BF16),
            vmem((1, width), F32),
            vmem((3, width, sub), BF16),
            vmem((sub, width), BF16),
            pltpu.SMEM(intersection.shape[::-1], I32),
            vmem((rows // lanes, lanes), I32),
            vmem((rows // lanes, lanes), I32),
            vmem((nl + 4, 2 * tok + 32, sub), BF16),
            vmem((nl, tok, sub), BF16),
            vmem((nl, 2, tok, sub), BF16),
            vmem((4, sub, sub), BF16),
            vmem((nl, tok, sub), BF16),
            vmem((nl, tok, sub), BF16),
            vmem((rows, sub), BF16),
            vmem((nv * cap, rows), BF16),
            vmem((rows, nv * cap), BF16),
            vmem((rows // lanes, lanes), F32),
            vmem((nv, 8, lanes), I32),
            vmem((nv, 8, lanes), I32),
            vmem((nv, cap, sub), BF16),
            vmem((nv, cap, sub), BF16),
            vmem((rows, sub), F32),
            vmem((nl, tok, width), BF16),
            vmem((sub, tok), F32),
            dma((12,)),
            dma((nl,)), dma((nl,)), dma((4,)), dma((4,)), dma((4,)), dma((4,)),
            dma((nl, 2)), dma((nl, 2)), dma((nl, 2)), dma((nl, 2)),
            dma((nv,)), dma((nv,)), dma((nv,)), dma((nv,)),
        ],
        compiler_params=pltpu.CompilerParams(
            collective_id=0, has_side_effects=True, vmem_limit_bytes=VMEM_MIB * 1024 * 1024
        ),
    )(
        latents,
        norm_gain.reshape(1, width),
        w_qkv,
        w_out,
        intersection.T,
        match_block.reshape(rows // lanes, lanes),
        match_row.reshape(rows // lanes, lanes),
    )
    mine = lay.astype(F32)
    refined = mine + COUPLING * (confidence[:, None] * (got.astype(F32) - mine))
    return refined.reshape(nl, tok, sub)


def solution(mesh):
    in_specs = (
        P("views", None, None),
        P(),
        P(None, None, "heads"),
        P("heads", None),
        P(),
        P("views", None),
        P("views"),
        P("views"),
    )
    out_specs = P("views", None, "heads")
    return jax.shard_map(
        functools.partial(per_device, mesh.shape["views"]),
        mesh=mesh, in_specs=in_specs, out_specs=out_specs, check_vma=False,
    )
```

```python
import functools

import jax
import jax.numpy as jnp
from jax import lax
from jax.experimental import pallas as pl
from jax.experimental.pallas import tpu as pltpu
from jax.sharding import PartitionSpec as P

MESH = pl.DeviceIdType.MESH
F32, BF16, I32 = jnp.float32, jnp.bfloat16, jnp.int32
EPSILON = 1e-06
COUPLING = 0.5
LOG2_E = 1.4426950408889634
HEAD_DIM = 64
ORDER = (1, 0, 2, 3)
SIDE = 4
VMEM_MIB = 60


def ring_steps(d):
    return min(d, SIDE - d)


PLACES = sorted(
    ((dx, dy, dc) for dx in range(SIDE) for dy in range(SIDE) for dc in range(2)),
    key=lambda p: (-ring_steps(p[0]) - ring_steps(p[1]), -p[2]),
)
PICK_GROUPS = ((0, 4), (4, 8), (8, 16), (16, 24), (24, 32))
TAKE_GROUPS = ((0, 8), (8, 16), (16, 24), (24, 28), (28, 32))


def dot(a, b):
    return jnp.dot(a, b, preferred_element_type=F32)


def dot_nt(a, b):
    return lax.dot_general(a, b, (((1,), (1,)), ((), ())), preferred_element_type=F32)


def value_rows(h):
    start = 256 + (2 * HEAD_DIM + 16) * (h // 2) + (h % 2) * HEAD_DIM
    return start, start + 16 * (h % 2)


def scope(name):
    return jax.named_scope(name)


def kernel(
    nv, views_total, cap,
    lat_h, gain_h, wqkv_h, wout_h, inter_h, mb_h, mr_h,
    lay_out, got_out,
    lat, gain, wqkv, wout, inter, mb, mr,
    kv, q, att, wo, part_s, part_r, lay, gsel, fsel, idxs, reqo, reqi, rows, reps, acc, normed, turned, got,
    in_sem, lay_sem, got_sem, kv_s, kv_r, wo_s, wo_r, ws_s, ws_r, at_s, at_r, pt_s, pt_r, rq_s, rq_r, rp_s, rp_r,
):
    nl, tok, width = lat.shape
    sub = wqkv.shape[2]
    me = lax.axis_index("views")
    z = lax.axis_index("heads")
    odd = lax.rem(z, 2)
    pair, opp = z + 1 - 2 * odd, lax.rem(z + 3 + 2 * odd, 4)
    far = lax.rem(z + 2, 4)
    px, py, pc = me // (2 * SIDE), lax.rem(me // 2, SIDE), lax.rem(me, 2)
    partner = me + 1 - 2 * pc
    beyond = lax.rem(me + nv - 1 + 2 * pc, nv)

    def actual(u):
        return u * pc + (nl - 1 - u) * (1 - pc)

    def away(o, sign):
        dx, dy, dc = PLACES[o]
        bx = lax.rem(px + (dx if sign > 0 else SIDE - dx), SIDE)
        by = lax.rem(py + (dy if sign > 0 else SIDE - dy), SIDE)
        return bx * (2 * SIDE) + by * 2 + lax.rem(pc + dc, 2)

    def load(n, src, dst):
        copy = pltpu.make_async_copy(src, dst, in_sem.at[n])
        copy.start()
        return copy

    in_gain = load(0, gain_h, gain)
    in_lat = {3: load(1, lat_h.at[actual(3)], lat.at[3])}
    in_k = load(2, wqkv_h.at[1], wqkv.at[1])
    in_v = load(3, wqkv_h.at[2], wqkv.at[2])
    for u in (2, 0, 1):
        in_lat[u] = load(6 + u, lat_h.at[actual(u)], lat.at[u])
    in_wout = load(5, wout_h, wout)
    in_q = load(4, wqkv_h.at[0], wqkv.at[0])
    in_small = [load(9, mb_h, mb), load(10, mr_h, mr), load(11, inter_h, inter)]

    def remote(src, dst, send, recv, device):
        return pltpu.make_async_remote_copy(
            src_ref=src, dst_ref=dst, send_sem=send, recv_sem=recv,
            device_id=device, device_id_type=MESH,
        )

    barrier = pltpu.get_barrier_semaphore()

    def greet(k, carry):
        pl.semaphore_signal(
            barrier, inc=1, device_id=(lax.rem(me + k, nv), z), device_id_type=MESH
        )
        return carry

    lax.fori_loop(1, nv, greet, 0)
    for other in (pair, opp):
        pl.semaphore_signal(barrier, inc=1, device_id=(me, other), device_id_type=MESH)

    def kv_copy(u):
        slot = (1, 0, nl + 3, nl + 2)[u]
        target = partner if u < 2 else beyond
        return remote(kv.at[2 + u], kv.at[slot], kv_s.at[u], kv_r.at[u], (target, z))

    half = sub // 2
    my_half = pl.ds(pl.multiple_of(pc * half, half), half)

    def wo_copy(n):
        cols = pl.ds(pl.multiple_of((pair, far, opp, far)[n] * sub, sub), sub)
        target = (pair, opp)[n // 2]
        return remote(
            wout.at[my_half, cols], wo.at[n, my_half], wo_s.at[n], wo_r.at[n], (me, target)
        )

    def wo_share(n):
        block = wo.at[n, my_half]
        return remote(block, block, ws_s.at[n], ws_r.at[n], (partner, z))

    def ways(n):
        return (opp, pair) if n % 2 == 0 else (pair, opp)

    def pieces(n):
        size = tok // 2 if n == nl - 1 else tok
        return [(c, pl.ds(c * size, size)) for c in range(tok // size)]

    def att_copy(n, c, part):
        return remote(
            att.at[n, 0, part], att.at[n, 1, part], at_s.at[n, c], at_r.at[n, c], (me, ways(n)[0])
        )

    def part_copy(n, c, part):
        return remote(
            part_s.at[n, part], part_r.at[n, part], pt_s.at[n, c], pt_r.at[n, c], (me, ways(n)[1])
        )

    def req_copy(o):
        return remote(reqo.at[o], reqi.at[o], rq_s.at[o], rq_r.at[o], (away(o, 1), z))

    def rep_copy(o):
        return remote(rows.at[o], reps.at[o], rp_s.at[o], rp_r.at[o], (away(o, -1), z))

    in_gain.wait()
    for n, u in enumerate((3, 2, 0, 1)):
        with scope(f"proj{n}"):
            in_lat[u].wait()
            wide = lat[u].astype(F32)
            mean_square = jnp.mean(wide * wide, axis=-1, keepdims=True)
            x = (wide * lax.rsqrt(mean_square + EPSILON) * gain[...]).astype(BF16)
            normed[u] = x
            if n == 0:
                in_k.wait()
            kv[2 + u, :tok, :] = dot(x, wqkv[1]).astype(BF16)
            if n == 0:
                in_v.wait()
            values = jnp.transpose(dot(x, wqkv[2])).astype(BF16)
            for h in range(sub // HEAD_DIM):
                top, first_row = value_rows(h)
                kv[2 + u, first_row : first_row + HEAD_DIM, :] = values[HEAD_DIM * h : HEAD_DIM * (h + 1)]
                if h % 2 == 0:
                    kv[2 + u, first_row + HEAD_DIM : first_row + HEAD_DIM + 16, :] = jnp.ones((16, tok), BF16)
        if n == 2:
            with scope("greeted"):
                pl.semaphore_wait(barrier, nv + 1)
            for early in (0, 3, 2):
                kv_copy(early).start()
            in_wout.wait()
            for k in range(4):
                wo_copy(k).start()
    kv_copy(1).start()
    in_q.wait()
    for copy in in_small:
        copy.wait()

    def ask(begin, end):
        found = dot(normed[begin:end].reshape((end - begin) * tok, width), wqkv[0])
        found = (found * (HEAD_DIM ** (-0.5) * LOG2_E)).astype(BF16)
        q[begin:end] = found.reshape(end - begin, tok, sub)

    lanes = mb.shape[1]

    def prepare():
        named = mb[...]
        rel = (((named >> 3) - px) & 3) * 8 + ((((named >> 1) & 3) - py) & 3) * 2 + ((named - pc) & 1)
        place = jnp.zeros_like(rel)
        for o, (dx, dy, dc) in enumerate(PLACES):
            place = jnp.where(rel == dx * 8 + dy * 2 + dc, o, place)
        wanted = mr[...]
        block_iota = lax.broadcasted_iota(I32, (nv, lanes), 0)
        slot_iota = lax.broadcasted_iota(I32, (lanes, lanes), 0)
        before = (slot_iota < lax.broadcasted_iota(I32, (lanes, lanes), 1)).astype(F32).astype(BF16)
        base = jnp.zeros((nv, 1), F32)
        digits = jnp.zeros((2 * nv, lanes), F32)
        for c in range(mb.shape[0]):
            onehot = (place[c : c + 1] == block_iota).astype(F32)
            earlier = dot(onehot.astype(BF16), before) + base
            slot = jnp.sum(onehot * earlier, axis=0, keepdims=True)
            base = base + jnp.sum(onehot, axis=1, keepdims=True)
            idxs[c : c + 1, :] = place[c : c + 1].astype(F32) * cap + slot
            is_slot = (slot.astype(I32) == slot_iota).astype(F32).astype(BF16)
            row = wanted[c : c + 1]
            high, low = (row >> 5).astype(F32), (row & 31).astype(F32)
            both = jnp.concatenate([onehot * high, onehot * low], axis=0).astype(BF16)
            digits = digits + dot_nt(both, is_slot)
        requests = (digits[:nv] * 32.0 + digits[nv:]).astype(I32)
        for k in range(nv):
            reqo[k] = jnp.broadcast_to(requests[k : k + 1], reqo.shape[1:])
        reqi[nv - 1] = jnp.broadcast_to(requests[nv - 1 : nv], reqo.shape[1:])
        for o in range(nv - 1):
            req_copy(o).start()

    lane = lax.broadcasted_iota(I32, (1, 2 * HEAD_DIM), 1)
    first = lane < HEAD_DIM

    def attend(n, i):
        a = me * nl + actual(i)
        bias = []
        for j in range(5):
            d = j - 2
            if d == 0:
                bias.append(None)
            else:
                back = d * (1 - pc) if d > 0 else -d * pc
                source = lax.rem(a - back + views_total, views_total)
                present = inter[abs(d) - 1, source]
                bias.append((1.0 - present.astype(F32)) * 1e30)
        heads = sub // HEAD_DIM
        scores = []
        for h in range(heads):
            cols = slice(2 * HEAD_DIM * (h // 2), 2 * HEAD_DIM * (h // 2 + 1))
            both = q[i, :, cols]
            mine = first if h % 2 == 0 else jnp.logical_not(first)
            query = jnp.where(mine, both, jnp.zeros_like(both))
            tiles = []
            for j in range(5):
                s = dot_nt(kv[i + j, :tok, cols], query)
                high = jnp.max(s.reshape(tok // 8, 8, tok), axis=0)
                tiles.append((s, high if bias[j] is None else high - bias[j]))
            scores.append(tiles)
        for h in range(heads):
            top = functools.reduce(jnp.maximum, [high for _, high in scores[h]])
            top = jnp.max(top, axis=0, keepdims=True)
            found = None
            begin, _ = value_rows(h)
            for j in range(5):
                p = jnp.exp2(scores[h][j][0] - (top if bias[j] is None else top + bias[j]))
                part = dot(kv[i + j, begin : begin + HEAD_DIM + 16, :], p.astype(BF16))
                found = part if found is None else found + part
            if h % 2 == 0:
                numer, total = found[:HEAD_DIM], found[HEAD_DIM : HEAD_DIM + 1]
            else:
                numer, total = found[16:], found[0:1]
            turned[HEAD_DIM * h : HEAD_DIM * (h + 1), :] = numer / total
        att[n, 0] = jnp.transpose(turned[...]).astype(BF16)

    own, to_pair, to_opp = (
        pl.ds(pl.multiple_of(g * sub, sub), sub) for g in (z, pair, opp)
    )

    def rounded(a, b):
        return dot(a, b).astype(BF16).astype(F32)

    def pass_on(n):
        cols, block = ((to_pair, 3), (to_opp, 1))[n % 2]
        for c, part in pieces(n):
            att_copy(n, c, part).wait_recv()
            summed = rounded(att[n, 0, part], wout[:, cols]) + rounded(att[n, 1, part], wo[block])
            part_s[n, part] = summed.astype(BF16)
            part_copy(n, c, part).start()

    def lay_copy(n):
        here = pl.ds(pl.multiple_of(actual(ORDER[n]) * tok, tok), tok)
        return pltpu.make_async_copy(lay.at[here], lay_out.at[here], lay_sem.at[n])

    def got_copy(c):
        here = pl.ds(c * tok, tok)
        return pltpu.make_async_copy(got.at[here], got_out.at[here], got_sem.at[c])

    def finish(n):
        u = ORDER[n]
        proj = rounded(att[n, 0], wout[:, own]) + rounded(att[n, 1], wo[2 - 2 * (n % 2)])
        for c, part in pieces(n):
            part_copy(n, c, part).wait_recv()
        proj = proj + part_r[n].astype(F32)
        done = (lat[u, :, own].astype(F32) + proj).astype(BF16)
        lay[pl.ds(pl.multiple_of(actual(u) * tok, tok), tok), :] = done

    n_slots = nv * cap

    def select_mine():
        places = jnp.transpose(idxs[...])
        for c in range(mb.shape[0]):
            at = places[:, c : c + 1].astype(I32)
            hit = at == lax.broadcasted_iota(I32, (lanes, n_slots), 1)
            fsel[lanes * c : lanes * (c + 1), :] = hit.astype(F32).astype(BF16)

    def select_asked():
        for o in range(nv - 1):
            req_copy(o).wait()
        asked = jnp.transpose(reqi[:, 0, :])
        for k in range(nv):
            hit = asked[:cap, k : k + 1] == lax.broadcasted_iota(I32, (cap, nl * tok), 1)
            gsel[cap * k : cap * (k + 1), :] = hit.astype(F32).astype(BF16)

    for n, u in enumerate(ORDER):
        with scope(f"halo{n}"):
            kv_copy((0, 1, 3, 2)[n]).wait_recv()
        with scope(f"att{n}"):
            if n == 0:
                ask(0, nl)
            attend(n, u)
        for c, part in pieces(n):
            att_copy(n, c, part).start()
        if n == 1:
            for k in range(4):
                wo_copy(k).wait()
                wo_share(k).start()

    with scope("wo"):
        for k in range(4):
            wo_share(k).wait()
    with scope("pass1"):
        pass_on(1)
    with scope("pass0"):
        pass_on(0)
    with scope("prep"):
        prepare()
    with scope("sel_mine"):
        select_mine()
    with scope("pass2"):
        pass_on(2)
    with scope("pass3"):
        pass_on(3)
    with scope("sel_asked"):
        select_asked()
    for n in range(nl):
        with scope(f"finish{n}"):
            finish(n)
            lay_copy(n).start()

    for lo, hi in PICK_GROUPS:
        with scope(f"pick{lo}"):
            picked = dot(gsel[cap * lo : cap * hi, :], lay[...]).astype(BF16)
            picked = picked.reshape(hi - lo, cap, sub)
            rows[lo:hi] = picked
            if hi == nv:
                reps[nv - 1] = picked[-1]
            for o in range(lo, min(hi, nv - 1)):
                rep_copy(o).start()

    for lo, hi in TAKE_GROUPS:
        with scope(f"take{lo}"):
            for o in range(lo, min(hi, nv - 1)):
                rep_copy(o).wait()
            block = reps[lo:hi].reshape((hi - lo) * cap, sub)
            if hi < nv:
                part = dot(fsel[:, cap * lo : cap * hi], block)
                acc[...] = part if lo == 0 else acc[...] + part
            else:
                for c in range(nl):
                    here = slice(c * tok, (c + 1) * tok)
                    part = dot(fsel[here, cap * lo : cap * hi], block)
                    got[here, :] = (acc[here, :] + part).astype(BF16)
                    got_copy(c).start()

    with scope("sent"):
        for i in range(nl):
            kv_copy(i).wait_send()
            for c, part in pieces(i):
                att_copy(i, c, part).wait_send()
                part_copy(i, c, part).wait_send()
    with scope("stored"):
        for c in range(nl):
            lay_copy(c).wait()
            got_copy(c).wait()


def blend(conf_h, lay_h, got_h, out_h, conf, lay, got, out, conf_sem, lay_sem, got_sem, out_sem):
    pieces, size, _ = lay.shape
    lanes = conf.shape[1]
    first = pltpu.make_async_copy(conf_h, conf, conf_sem.at[0])
    first.start()
    loads, stores = [], []
    for c in range(pieces):
        here = pl.ds(c * size, size)
        loads.append(
            (
                pltpu.make_async_copy(lay_h.at[here], lay.at[c], lay_sem.at[c]),
                pltpu.make_async_copy(got_h.at[here], got.at[c], got_sem.at[c]),
            )
        )
        stores.append(pltpu.make_async_copy(out.at[c], out_h.at[here], out_sem.at[c]))
        for copy in loads[c]:
            copy.start()
    first.wait()
    weight = COUPLING * jnp.transpose(conf[...])
    for c in range(pieces):
        for copy in loads[c]:
            copy.wait()
        for k in range(size // lanes):
            here = pl.ds(k * lanes, lanes)
            mine = lay[c, here].astype(F32)
            column = c * (size // lanes) + k
            other = got[c, here].astype(F32)
            out[c, here] = mine + weight[:, column : column + 1] * (other - mine)
        stores[c].start()
    for copy in stores:
        copy.wait()


def per_device(nv, latents, norm_gain, w_qkv, w_out, intersection, match_block, match_row, confidence):
    nl, tok, width = latents.shape
    sub = w_qkv.shape[2]
    rows = nl * tok
    cap = 2 * rows // nv
    here = pl.BlockSpec(memory_space=pltpu.HBM)
    dma = pltpu.SemaphoreType.DMA
    vmem = pltpu.VMEM
    lanes = 128
    lay, got = pl.pallas_call(
        functools.partial(kernel, nv, nl * nv, cap),
        out_shape=[jax.ShapeDtypeStruct((rows, sub), BF16)] * 2,
        in_specs=[here] * 7,
        out_specs=[here] * 2,
        scratch_shapes=[
            vmem((nl, tok, width), BF16),
            vmem((1, width), F32),
            vmem((3, width, sub), BF16),
            vmem((sub, width), BF16),
            pltpu.SMEM(intersection.shape[::-1], I32),
            vmem((rows // lanes, lanes), I32),
            vmem((rows // lanes, lanes), I32),
            vmem((nl + 4, 2 * tok + 32, sub), BF16),
            vmem((nl, tok, sub), BF16),
            vmem((nl, 2, tok, sub), BF16),
            vmem((4, sub, sub), BF16),
            vmem((nl, tok, sub), BF16),
            vmem((nl, tok, sub), BF16),
            vmem((rows, sub), BF16),
            vmem((nv * cap, rows), BF16),
            vmem((rows, nv * cap), BF16),
            vmem((rows // lanes, lanes), F32),
            vmem((nv, 8, lanes), I32),
            vmem((nv, 8, lanes), I32),
            vmem((nv, cap, sub), BF16),
            vmem((nv, cap, sub), BF16),
            vmem((rows, sub), F32),
            vmem((nl, tok, width), BF16),
            vmem((sub, tok), F32),
            vmem((rows, sub), BF16),
            dma((12,)), dma((nl,)), dma((nl,)),
            dma((nl,)), dma((nl,)), dma((4,)), dma((4,)), dma((4,)), dma((4,)),
            dma((nl, 2)), dma((nl, 2)), dma((nl, 2)), dma((nl, 2)),
            dma((nv,)), dma((nv,)), dma((nv,)), dma((nv,)),
        ],
        compiler_params=pltpu.CompilerParams(
            collective_id=0, has_side_effects=True, vmem_limit_bytes=VMEM_MIB * 1024 * 1024
        ),
    )(
        latents,
        norm_gain.reshape(1, width),
        w_qkv,
        w_out,
        intersection.T,
        match_block.reshape(rows // lanes, lanes),
        match_row.reshape(rows // lanes, lanes),
    )
    pieces = 4
    refined = pl.pallas_call(
        blend,
        out_shape=jax.ShapeDtypeStruct((rows, sub), F32),
        in_specs=[here] * 3,
        out_specs=here,
        scratch_shapes=[
            vmem((rows // lanes, lanes), F32),
            vmem((pieces, rows // pieces, sub), BF16),
            vmem((pieces, rows // pieces, sub), BF16),
            vmem((pieces, rows // pieces, sub), F32),
            dma((1,)), dma((pieces,)), dma((pieces,)), dma((pieces,)),
        ],
    )(confidence.reshape(rows // lanes, lanes), lay, got)
    return refined.reshape(nl, tok, sub)


def solution(mesh):
    in_specs = (
        P("views", None, None),
        P(),
        P(None, None, "heads"),
        P("heads", None),
        P(),
        P("views", None),
        P("views"),
        P("views"),
    )
    out_specs = P("views", None, "heads")
    return jax.shard_map(
        functools.partial(per_device, mesh.shape["views"]),
        mesh=mesh, in_specs=in_specs, out_specs=out_specs, check_vma=False,
    )
```

```python
import functools

import jax
import jax.numpy as jnp
from jax import lax
from jax.experimental import pallas as pl
from jax.experimental.pallas import tpu as pltpu
from jax.sharding import PartitionSpec as P

MESH = pl.DeviceIdType.MESH
F32, BF16, I32 = jnp.float32, jnp.bfloat16, jnp.int32
EPSILON = 1e-06
COUPLING = 0.5
LOG2_E = 1.4426950408889634
HEAD_DIM = 64
ORDER = (1, 0, 2, 3)
SIDE = 4
VMEM_MIB = 60


def ring_steps(d):
    return min(d, SIDE - d)


PLACES = sorted(
    ((dx, dy, dc) for dx in range(SIDE) for dy in range(SIDE) for dc in range(2)),
    key=lambda p: (-ring_steps(p[0]) - ring_steps(p[1]), -p[2]),
)
PICK_GROUPS = ((0, 4), (4, 8), (8, 16), (16, 24), (24, 32))
TAKE_GROUPS = ((0, 8), (8, 16), (16, 24), (24, 32))


def dot(a, b):
    return jnp.dot(a, b, preferred_element_type=F32)


def dot_nt(a, b):
    return lax.dot_general(a, b, (((1,), (1,)), ((), ())), preferred_element_type=F32)


def value_rows(h):
    start = 256 + (2 * HEAD_DIM + 16) * (h // 2) + (h % 2) * HEAD_DIM
    return start, start + 16 * (h % 2)


def scope(name):
    return jax.named_scope(name)


def kernel(
    nv, views_total, cap,
    lat_h, gain_h, wqkv_h, wout_h, inter_h, mb_h, mr_h,
    lay_out, got_out,
    lat, gain, wqkv, wout, inter, mb, mr,
    kv, q, att, wo, part_s, part_r, lay, gsel, fsel, idxs, reqo, reqi, rows, reps, acc, normed, turned, got, base,
    in_sem, lay_sem, got_sem, kv_s, kv_r, wo_s, wo_r, ws_s, ws_r, at_s, at_r, pt_s, pt_r, rq_s, rq_r, rp_s, rp_r,
):
    nl, tok, width = lat.shape
    sub = wqkv.shape[2]
    me = lax.axis_index("views")
    z = lax.axis_index("heads")
    odd = lax.rem(z, 2)
    pair, opp = z + 1 - 2 * odd, lax.rem(z + 3 + 2 * odd, 4)
    far = lax.rem(z + 2, 4)
    px, py, pc = me // (2 * SIDE), lax.rem(me // 2, SIDE), lax.rem(me, 2)
    partner = me + 1 - 2 * pc
    beyond = lax.rem(me + nv - 1 + 2 * pc, nv)

    def actual(u):
        return u * pc + (nl - 1 - u) * (1 - pc)

    def away(o, sign):
        dx, dy, dc = PLACES[o]
        bx = lax.rem(px + (dx if sign > 0 else SIDE - dx), SIDE)
        by = lax.rem(py + (dy if sign > 0 else SIDE - dy), SIDE)
        return bx * (2 * SIDE) + by * 2 + lax.rem(pc + dc, 2)

    def load(n, src, dst):
        copy = pltpu.make_async_copy(src, dst, in_sem.at[n])
        copy.start()
        return copy

    in_gain = load(0, gain_h, gain)
    in_lat = {3: load(1, lat_h.at[actual(3)], lat.at[3])}
    in_k = load(2, wqkv_h.at[1], wqkv.at[1])
    in_v = load(3, wqkv_h.at[2], wqkv.at[2])
    for u in (2, 0, 1):
        in_lat[u] = load(6 + u, lat_h.at[actual(u)], lat.at[u])
    in_wout = load(5, wout_h, wout)
    in_q = load(4, wqkv_h.at[0], wqkv.at[0])
    in_small = [load(9, mb_h, mb), load(10, mr_h, mr), load(11, inter_h, inter)]

    def remote(src, dst, send, recv, device):
        return pltpu.make_async_remote_copy(
            src_ref=src, dst_ref=dst, send_sem=send, recv_sem=recv,
            device_id=device, device_id_type=MESH,
        )

    barrier = pltpu.get_barrier_semaphore()

    def greet(k, carry):
        pl.semaphore_signal(
            barrier, inc=1, device_id=(lax.rem(me + k, nv), z), device_id_type=MESH
        )
        return carry

    lax.fori_loop(1, nv, greet, 0)
    for other in (pair, opp):
        pl.semaphore_signal(barrier, inc=1, device_id=(me, other), device_id_type=MESH)

    def kv_copy(u):
        slot = (1, 0, nl + 3, nl + 2)[u]
        target = partner if u < 2 else beyond
        return remote(kv.at[2 + u], kv.at[slot], kv_s.at[u], kv_r.at[u], (target, z))

    half = sub // 2
    my_half = pl.ds(pl.multiple_of(pc * half, half), half)

    def wo_copy(n):
        cols = pl.ds(pl.multiple_of((pair, far, opp, far)[n] * sub, sub), sub)
        target = (pair, opp)[n // 2]
        return remote(
            wout.at[my_half, cols], wo.at[n, my_half], wo_s.at[n], wo_r.at[n], (me, target)
        )

    def wo_share(n):
        block = wo.at[n, my_half]
        return remote(block, block, ws_s.at[n], ws_r.at[n], (partner, z))

    def ways(n):
        return (opp, pair) if n % 2 == 0 else (pair, opp)

    def pieces(n):
        size = tok // 2 if n == nl - 1 else tok
        return [(c, pl.ds(c * size, size)) for c in range(tok // size)]

    def att_copy(n, c, part):
        return remote(
            att.at[n, 0, part], att.at[n, 1, part], at_s.at[n, c], at_r.at[n, c], (me, ways(n)[0])
        )

    def part_copy(n, f, c, part):
        return remote(
            part_s.at[f, n, part], part_r.at[f, n, part],
            pt_s.at[n, 2 * f + c], pt_r.at[n, 2 * f + c], (me, ways(n)[1]),
        )

    def req_copy(o):
        return remote(reqo.at[o], reqi.at[o], rq_s.at[o], rq_r.at[o], (away(o, 1), z))

    def rep_copy(f, o):
        return remote(
            rows.at[f, o], reps.at[f, o], rp_s.at[f, o], rp_r.at[f, o], (away(o, -1), z)
        )

    fw = sub // 2
    halves = (slice(0, fw), slice(fw, sub))

    lanes = mb.shape[1]

    def prepare():
        named = mb[...]
        rel = (((named >> 3) - px) & 3) * 8 + ((((named >> 1) & 3) - py) & 3) * 2 + ((named - pc) & 1)
        place = jnp.zeros_like(rel)
        for o, (dx, dy, dc) in enumerate(PLACES):
            place = jnp.where(rel == dx * 8 + dy * 2 + dc, o, place)
        wanted = mr[...]
        block_iota = lax.broadcasted_iota(I32, (nv, lanes), 0)
        slot_iota = lax.broadcasted_iota(I32, (lanes, lanes), 0)
        before = (slot_iota < lax.broadcasted_iota(I32, (lanes, lanes), 1)).astype(F32).astype(BF16)
        base = jnp.zeros((nv, 1), F32)
        digits = jnp.zeros((2 * nv, lanes), F32)
        for c in range(mb.shape[0]):
            onehot = (place[c : c + 1] == block_iota).astype(F32)
            earlier = dot(onehot.astype(BF16), before) + base
            slot = jnp.sum(onehot * earlier, axis=0, keepdims=True)
            base = base + jnp.sum(onehot, axis=1, keepdims=True)
            idxs[c : c + 1, :] = place[c : c + 1].astype(F32) * cap + slot
            is_slot = (slot.astype(I32) == slot_iota).astype(F32).astype(BF16)
            row = wanted[c : c + 1]
            high, low = (row >> 5).astype(F32), (row & 31).astype(F32)
            both = jnp.concatenate([onehot * high, onehot * low], axis=0).astype(BF16)
            digits = digits + dot_nt(both, is_slot)
        requests = (digits[:nv] * 32.0 + digits[nv:]).astype(I32)
        for k in range(nv):
            reqo[k] = jnp.broadcast_to(requests[k : k + 1], reqo.shape[1:])
        reqi[nv - 1] = jnp.broadcast_to(requests[nv - 1 : nv], reqo.shape[1:])

    in_gain.wait()
    for n, u in enumerate((3, 2, 0, 1)):
        with scope(f"proj{n}"):
            in_lat[u].wait()
            wide = lat[u].astype(F32)
            mean_square = jnp.mean(wide * wide, axis=-1, keepdims=True)
            x = (wide * lax.rsqrt(mean_square + EPSILON) * gain[...]).astype(BF16)
            normed[u] = x
            if n == 0:
                in_k.wait()
            kv[2 + u, :tok, :] = dot(x, wqkv[1]).astype(BF16)
            if n == 0:
                in_v.wait()
            values = jnp.transpose(dot(x, wqkv[2])).astype(BF16)
            for h in range(sub // HEAD_DIM):
                top, first_row = value_rows(h)
                kv[2 + u, first_row : first_row + HEAD_DIM, :] = values[HEAD_DIM * h : HEAD_DIM * (h + 1)]
                if h % 2 == 0:
                    kv[2 + u, first_row + HEAD_DIM : first_row + HEAD_DIM + 16, :] = jnp.ones((16, tok), BF16)
        if n == 2:
            with scope("prep"):
                for copy in in_small:
                    copy.wait()
                prepare()
            with scope("greeted"):
                pl.semaphore_wait(barrier, nv + 1)
            for early in (0, 3, 2):
                kv_copy(early).start()
            in_wout.wait()
            for k in range(4):
                wo_copy(k).start()
    kv_copy(1).start()
    in_q.wait()
    def ask(begin, end):
        found = dot(normed[begin:end].reshape((end - begin) * tok, width), wqkv[0])
        found = (found * (HEAD_DIM ** (-0.5) * LOG2_E)).astype(BF16)
        q[begin:end] = found.reshape(end - begin, tok, sub)

    lane = lax.broadcasted_iota(I32, (1, 2 * HEAD_DIM), 1)
    first = lane < HEAD_DIM

    def attend(n, i):
        a = me * nl + actual(i)
        bias = []
        for j in range(5):
            d = j - 2
            if d == 0:
                bias.append(None)
            else:
                back = d * (1 - pc) if d > 0 else -d * pc
                source = lax.rem(a - back + views_total, views_total)
                present = inter[abs(d) - 1, source]
                bias.append((1.0 - present.astype(F32)) * 1e30)
        heads = sub // HEAD_DIM
        scores = []
        for h in range(heads):
            cols = slice(2 * HEAD_DIM * (h // 2), 2 * HEAD_DIM * (h // 2 + 1))
            both = q[i, :, cols]
            mine = first if h % 2 == 0 else jnp.logical_not(first)
            query = jnp.where(mine, both, jnp.zeros_like(both))
            tiles = []
            for j in range(5):
                s = dot_nt(kv[i + j, :tok, cols], query)
                high = jnp.max(s.reshape(tok // 8, 8, tok), axis=0)
                tiles.append((s, high if bias[j] is None else high - bias[j]))
            scores.append(tiles)
        for h in range(heads):
            top = functools.reduce(jnp.maximum, [high for _, high in scores[h]])
            top = jnp.max(top, axis=0, keepdims=True)
            found = None
            begin, _ = value_rows(h)
            for j in range(5):
                p = jnp.exp2(scores[h][j][0] - (top if bias[j] is None else top + bias[j]))
                part = dot(kv[i + j, begin : begin + HEAD_DIM + 16, :], p.astype(BF16))
                found = part if found is None else found + part
            if h % 2 == 0:
                numer, total = found[:HEAD_DIM], found[HEAD_DIM : HEAD_DIM + 1]
            else:
                numer, total = found[16:], found[0:1]
            turned[HEAD_DIM * h : HEAD_DIM * (h + 1), :] = numer / total
        att[n, 0] = jnp.transpose(turned[...]).astype(BF16)

    own, to_pair, to_opp = (
        pl.ds(pl.multiple_of(g * sub, sub), sub) for g in (z, pair, opp)
    )

    def rounded(a, b):
        return dot(a, b).astype(BF16).astype(F32)

    def pass_on(n):
        cols, block = ((to_pair, 3), (to_opp, 1))[n % 2]
        for c, part in pieces(n):
            att_copy(n, c, part).wait_recv()
            summed = rounded(att[n, 0, part], wout[:, cols]) + rounded(att[n, 1, part], wo[block])
            for f in (0, 1):
                part_s[f, n, part] = summed[:, halves[f]].astype(BF16)
            part_copy(n, 0, c, part).start()
            if n == 1:
                part_copy(n, 1, c, part).start()

    def lay_copy(n, f):
        here = pl.ds(pl.multiple_of(actual(ORDER[n]) * tok, tok), tok)
        return pltpu.make_async_copy(
            lay.at[f, here], lay_out.at[here, halves[f]], lay_sem.at[n, f]
        )

    def got_copy(c):
        here = pl.ds(c * tok, tok)
        return pltpu.make_async_copy(got.at[here], got_out.at[here], got_sem.at[c])

    def begin(n):
        proj = rounded(att[n, 0], wout[:, own]) + rounded(att[n, 1], wo[2 - 2 * (n % 2)])
        base[n] = proj

    def finish(n, f):
        u = ORDER[n]
        mine = pl.ds(pl.multiple_of(z * sub + f * fw, fw), fw)
        for c, part in pieces(n):
            part_copy(n, f, c, part).wait_recv()
        proj = base[n, :, halves[f]] + part_r[f, n].astype(F32)
        done = (lat[u, :, mine].astype(F32) + proj).astype(BF16)
        lay[f, pl.ds(pl.multiple_of(actual(u) * tok, tok), tok), :] = done
        lay_copy(n, f).start()

    n_slots = nv * cap

    def select_mine():
        places = jnp.transpose(idxs[...])
        for c in range(mb.shape[0]):
            at = places[:, c : c + 1].astype(I32)
            hit = at == lax.broadcasted_iota(I32, (lanes, n_slots), 1)
            fsel[lanes * c : lanes * (c + 1), :] = hit.astype(F32).astype(BF16)

    def select_asked():
        for o in range(nv - 1):
            req_copy(o).wait()
        asked = jnp.transpose(reqi[:, 0, :])
        for k in range(nv):
            hit = asked[:cap, k : k + 1] == lax.broadcasted_iota(I32, (cap, nl * tok), 1)
            gsel[cap * k : cap * (k + 1), :] = hit.astype(F32).astype(BF16)

    for n, u in enumerate(ORDER):
        with scope(f"halo{n}"):
            kv_copy((0, 1, 3, 2)[n]).wait_recv()
        with scope(f"att{n}"):
            if n == 0:
                ask(0, nl)
            attend(n, u)
        for c, part in pieces(n):
            att_copy(n, c, part).start()
        if n == 1:
            for o in range(nv - 1):
                req_copy(o).start()
            for k in range(4):
                wo_copy(k).wait()
                wo_share(k).start()

    with scope("wo"):
        for k in range(4):
            wo_share(k).wait()
    with scope("pass1"):
        pass_on(1)
    with scope("pass0"):
        pass_on(0)
    with scope("sel_asked"):
        select_asked()
    with scope("pass2"):
        pass_on(2)
    with scope("pass3"):
        pass_on(3)
    for n in (0, 2, 3):
        for c, part in pieces(n):
            part_copy(n, 1, c, part).start()
    with scope("sel_mine"):
        select_mine()
    with scope("begin"):
        for n in range(nl):
            begin(n)

    for f in (0, 1):
        for n in range(nl):
            with scope(f"finish{f}{n}"):
                finish(n, f)
        for lo, hi in PICK_GROUPS:
            with scope(f"pick{f}{lo}"):
                picked = dot(gsel[cap * lo : cap * hi, :], lay[f]).astype(BF16)
                picked = picked.reshape(hi - lo, cap, fw)
                rows[f, lo:hi] = picked
                if hi == nv:
                    reps[f, nv - 1] = picked[-1]
                for o in range(lo, min(hi, nv - 1)):
                    rep_copy(f, o).start()

    for f in (0, 1):
        for lo, hi in TAKE_GROUPS:
            with scope(f"take{f}{lo}"):
                for o in range(lo, min(hi, nv - 1)):
                    rep_copy(f, o).wait()
                block = reps[f, lo:hi].reshape((hi - lo) * cap, fw)
                if hi < nv:
                    part = dot(fsel[:, cap * lo : cap * hi], block)
                    acc[...] = part if lo == 0 else acc[...] + part
                else:
                    for c in range(nl):
                        here = slice(c * tok, (c + 1) * tok)
                        part = dot(fsel[here, cap * lo : cap * hi], block)
                        got[here, halves[f]] = (acc[here, :] + part).astype(BF16)
                        if f == 1:
                            got_copy(c).start()

    with scope("sent"):
        for i in range(nl):
            kv_copy(i).wait_send()
            for c, part in pieces(i):
                att_copy(i, c, part).wait_send()
                for f in (0, 1):
                    part_copy(i, f, c, part).wait_send()
    with scope("stored"):
        for c in range(nl):
            for f in (0, 1):
                lay_copy(c, f).wait()
            got_copy(c).wait()


def blend(conf_h, lay_h, got_h, out_h, conf, lay, got, out, conf_sem, lay_sem, got_sem, out_sem):
    pieces, size, _ = lay.shape
    lanes = conf.shape[1]
    first = pltpu.make_async_copy(conf_h, conf, conf_sem.at[0])
    first.start()
    loads, stores = [], []
    for c in range(pieces):
        here = pl.ds(c * size, size)
        loads.append(
            (
                pltpu.make_async_copy(lay_h.at[here], lay.at[c], lay_sem.at[c]),
                pltpu.make_async_copy(got_h.at[here], got.at[c], got_sem.at[c]),
            )
        )
        stores.append(pltpu.make_async_copy(out.at[c], out_h.at[here], out_sem.at[c]))
        for copy in loads[c]:
            copy.start()
    first.wait()
    weight = COUPLING * jnp.transpose(conf[...])
    for c in range(pieces):
        for copy in loads[c]:
            copy.wait()
        for k in range(size // lanes):
            here = pl.ds(k * lanes, lanes)
            mine = lay[c, here].astype(F32)
            column = c * (size // lanes) + k
            other = got[c, here].astype(F32)
            out[c, here] = mine + weight[:, column : column + 1] * (other - mine)
        stores[c].start()
    for copy in stores:
        copy.wait()


def per_device(nv, latents, norm_gain, w_qkv, w_out, intersection, match_block, match_row, confidence):
    nl, tok, width = latents.shape
    sub = w_qkv.shape[2]
    rows = nl * tok
    cap = 2 * rows // nv
    here = pl.BlockSpec(memory_space=pltpu.HBM)
    dma = pltpu.SemaphoreType.DMA
    vmem = pltpu.VMEM
    lanes = 128
    lay, got = pl.pallas_call(
        functools.partial(kernel, nv, nl * nv, cap),
        out_shape=[jax.ShapeDtypeStruct((rows, sub), BF16)] * 2,
        in_specs=[here] * 7,
        out_specs=[here] * 2,
        scratch_shapes=[
            vmem((nl, tok, width), BF16),
            vmem((1, width), F32),
            vmem((3, width, sub), BF16),
            vmem((sub, width), BF16),
            pltpu.SMEM(intersection.shape[::-1], I32),
            vmem((rows // lanes, lanes), I32),
            vmem((rows // lanes, lanes), I32),
            vmem((nl + 4, 2 * tok + 32, sub), BF16),
            vmem((nl, tok, sub), BF16),
            vmem((nl, 2, tok, sub), BF16),
            vmem((4, sub, sub), BF16),
            vmem((2, nl, tok, sub // 2), BF16),
            vmem((2, nl, tok, sub // 2), BF16),
            vmem((2, rows, sub // 2), BF16),
            vmem((nv * cap, rows), BF16),
            vmem((rows, nv * cap), BF16),
            vmem((rows // lanes, lanes), F32),
            vmem((nv, 8, lanes), I32),
            vmem((nv, 8, lanes), I32),
            vmem((2, nv, cap, sub // 2), BF16),
            vmem((2, nv, cap, sub // 2), BF16),
            vmem((rows, sub // 2), F32),
            vmem((nl, tok, width), BF16),
            vmem((sub, tok), F32),
            vmem((rows, sub), BF16),
            vmem((nl, tok, sub), F32),
            dma((12,)), dma((nl, 2)), dma((nl,)),
            dma((nl,)), dma((nl,)), dma((4,)), dma((4,)), dma((4,)), dma((4,)),
            dma((nl, 2)), dma((nl, 2)), dma((nl, 4)), dma((nl, 4)),
            dma((nv,)), dma((nv,)), dma((2, nv)), dma((2, nv)),
        ],
        compiler_params=pltpu.CompilerParams(
            collective_id=0, has_side_effects=True, vmem_limit_bytes=VMEM_MIB * 1024 * 1024
        ),
    )(
        latents,
        norm_gain.reshape(1, width),
        w_qkv,
        w_out,
        intersection.T,
        match_block.reshape(rows // lanes, lanes),
        match_row.reshape(rows // lanes, lanes),
    )
    pieces = 4
    refined = pl.pallas_call(
        blend,
        out_shape=jax.ShapeDtypeStruct((rows, sub), F32),
        in_specs=[here] * 3,
        out_specs=here,
        scratch_shapes=[
            vmem((rows // lanes, lanes), F32),
            vmem((pieces, rows // pieces, sub), BF16),
            vmem((pieces, rows // pieces, sub), BF16),
            vmem((pieces, rows // pieces, sub), F32),
            dma((1,)), dma((pieces,)), dma((pieces,)), dma((pieces,)),
        ],
    )(confidence.reshape(rows // lanes, lanes), lay, got)
    return refined.reshape(nl, tok, sub)


def solution(mesh):
    in_specs = (
        P("views", None, None),
        P(),
        P(None, None, "heads"),
        P("heads", None),
        P(),
        P("views", None),
        P("views"),
        P("views"),
    )
    out_specs = P("views", None, "heads")
    return jax.shard_map(
        functools.partial(per_device, mesh.shape["views"]),
        mesh=mesh, in_specs=in_specs, out_specs=out_specs, check_vma=False,
    )
```

```python
import functools

import jax
import jax.numpy as jnp
from jax import lax
from jax.experimental import pallas as pl
from jax.experimental.pallas import tpu as pltpu
from jax.sharding import PartitionSpec as P

MESH = pl.DeviceIdType.MESH
F32, BF16, I32 = jnp.float32, jnp.bfloat16, jnp.int32
EPSILON = 1e-06
COUPLING = 0.5
LOG2_E = 1.4426950408889634
HEAD_DIM = 64
ORDER = (1, 0, 2, 3)
SIDE = 4
VMEM_MIB = 60


def ring_steps(d):
    return min(d, SIDE - d)


PLACES = sorted(
    ((dx, dy, dc) for dx in range(SIDE) for dy in range(SIDE) for dc in range(2)),
    key=lambda p: (-ring_steps(p[0]) - ring_steps(p[1]), -p[2]),
)
PICK_GROUPS = ((0, 4), (4, 8), (8, 16), (16, 24), (24, 32))
GROUP = 8
TAKE_GROUPS = ((0, 8), (8, 16), (16, 24), (24, 32))


def dot(a, b):
    return jnp.dot(a, b, preferred_element_type=F32)


def dot_nt(a, b):
    return lax.dot_general(a, b, (((1,), (1,)), ((), ())), preferred_element_type=F32)


def value_rows(h):
    start = 256 + (2 * HEAD_DIM + 16) * (h // 2) + (h % 2) * HEAD_DIM
    return start, start + 16 * (h % 2)


def scope(name):
    return jax.named_scope(name)


def kernel(
    nv, views_total, cap,
    lat_h, gain_h, wqkv_h, wout_h, inter_h, mb_h, mr_h,
    lay_out, got_out,
    lat, gain, wqkv, wout, inter, mb, mr,
    kv, q, att, wo, part_s, part_r, lay, gsel, fsel, idxs, reqo, reqi, rows, reps, acc, normed, turned, got, base,
    in_sem, lay_sem, got_sem, kv_s, kv_r, wo_s, wo_r, ws_s, ws_r, at_s, at_r, pt_s, pt_r, rq_s, rq_r, rp_s, rp_r,
):
    nl, tok, width = lat.shape
    sub = wqkv.shape[2]
    me = lax.axis_index("views")
    z = lax.axis_index("heads")
    odd = lax.rem(z, 2)
    pair, opp = z + 1 - 2 * odd, lax.rem(z + 3 + 2 * odd, 4)
    far = lax.rem(z + 2, 4)
    px, py, pc = me // (2 * SIDE), lax.rem(me // 2, SIDE), lax.rem(me, 2)
    partner = me + 1 - 2 * pc
    beyond = lax.rem(me + nv - 1 + 2 * pc, nv)

    def actual(u):
        return u * pc + (nl - 1 - u) * (1 - pc)

    def away(o, sign):
        dx, dy, dc = PLACES[o]
        bx = lax.rem(px + (dx if sign > 0 else SIDE - dx), SIDE)
        by = lax.rem(py + (dy if sign > 0 else SIDE - dy), SIDE)
        return bx * (2 * SIDE) + by * 2 + lax.rem(pc + dc, 2)

    def load(n, src, dst):
        copy = pltpu.make_async_copy(src, dst, in_sem.at[n])
        copy.start()
        return copy

    in_gain = load(0, gain_h, gain)
    in_lat = {3: load(1, lat_h.at[actual(3)], lat.at[3])}
    in_k = load(2, wqkv_h.at[1], wqkv.at[1])
    in_v = load(3, wqkv_h.at[2], wqkv.at[2])
    for u in (2, 0, 1):
        in_lat[u] = load(6 + u, lat_h.at[actual(u)], lat.at[u])
    in_wout = load(5, wout_h, wout)
    in_q = load(4, wqkv_h.at[0], wqkv.at[0])
    in_small = [load(9, mb_h, mb), load(10, mr_h, mr), load(11, inter_h, inter)]

    def remote(src, dst, send, recv, device):
        return pltpu.make_async_remote_copy(
            src_ref=src, dst_ref=dst, send_sem=send, recv_sem=recv,
            device_id=device, device_id_type=MESH,
        )

    barrier = pltpu.get_barrier_semaphore()

    def greet(k, carry):
        pl.semaphore_signal(
            barrier, inc=1, device_id=(lax.rem(me + k, nv), z), device_id_type=MESH
        )
        return carry

    lax.fori_loop(1, nv, greet, 0)
    for other in (pair, opp):
        pl.semaphore_signal(barrier, inc=1, device_id=(me, other), device_id_type=MESH)

    def kv_copy(u):
        slot = (1, 0, nl + 3, nl + 2)[u]
        target = partner if u < 2 else beyond
        return remote(kv.at[2 + u], kv.at[slot], kv_s.at[u], kv_r.at[u], (target, z))

    half = sub // 2
    my_half = pl.ds(pl.multiple_of(pc * half, half), half)

    def wo_copy(n):
        cols = pl.ds(pl.multiple_of((pair, far, opp, far)[n] * sub, sub), sub)
        target = (pair, opp)[n // 2]
        return remote(
            wout.at[my_half, cols], wo.at[n, my_half], wo_s.at[n], wo_r.at[n], (me, target)
        )

    def wo_share(n):
        block = wo.at[n, my_half]
        return remote(block, block, ws_s.at[n], ws_r.at[n], (partner, z))

    def ways(n):
        return (opp, pair) if n % 2 == 0 else (pair, opp)

    def pieces(n):
        size = tok // 2 if n == nl - 1 else tok
        return [(c, pl.ds(c * size, size)) for c in range(tok // size)]

    def att_copy(n, c, part):
        return remote(
            att.at[n, 0, part], att.at[n, 1, part], at_s.at[n + c], at_r.at[n + c], (me, ways(n)[0])
        )

    def part_copy(n, f, c, part):
        return remote(
            part_s.at[f, n, part], part_r.at[f, n, part],
            pt_s.at[f, n + c], pt_r.at[f, n + c], (me, ways(n)[1]),
        )

    def req_copy(o):
        return remote(reqo.at[o], reqi.at[o], rq_s.at[0], rq_r.at[0], (away(o, 1), z))

    def all_requests():
        here = pl.ds(0, nv - 1)
        return remote(reqo.at[here], reqi.at[here], rq_s.at[0], rq_r.at[0], (beyond, z))

    def rep_copy(f, o):
        g = o // GROUP
        return remote(
            rows.at[f, o], reps.at[f, o], rp_s.at[f, g], rp_r.at[f, g], (away(o, -1), z)
        )

    def reply_group(f, g):
        here = pl.ds(g * GROUP, min(GROUP, nv - 1 - g * GROUP))
        return remote(
            rows.at[f, here], reps.at[f, here], rp_s.at[f, g], rp_r.at[f, g], (beyond, z)
        )

    fw = sub // 2
    halves = (slice(0, fw), slice(fw, sub))

    lanes = mb.shape[1]

    def prepare():
        named = mb[...]
        rel = (((named >> 3) - px) & 3) * 8 + ((((named >> 1) & 3) - py) & 3) * 2 + ((named - pc) & 1)
        place = jnp.zeros_like(rel)
        for o, (dx, dy, dc) in enumerate(PLACES):
            place = jnp.where(rel == dx * 8 + dy * 2 + dc, o, place)
        wanted = mr[...]
        block_iota = lax.broadcasted_iota(I32, (nv, lanes), 0)
        slot_iota = lax.broadcasted_iota(I32, (lanes, lanes), 0)
        before = (slot_iota < lax.broadcasted_iota(I32, (lanes, lanes), 1)).astype(F32).astype(BF16)
        base = jnp.zeros((nv, 1), F32)
        digits = jnp.zeros((2 * nv, lanes), F32)
        for c in range(mb.shape[0]):
            onehot = (place[c : c + 1] == block_iota).astype(F32)
            earlier = dot(onehot.astype(BF16), before) + base
            slot = jnp.sum(onehot * earlier, axis=0, keepdims=True)
            base = base + jnp.sum(onehot, axis=1, keepdims=True)
            idxs[c : c + 1, :] = place[c : c + 1].astype(F32) * cap + slot
            is_slot = (slot.astype(I32) == slot_iota).astype(F32).astype(BF16)
            row = wanted[c : c + 1]
            high, low = (row >> 5).astype(F32), (row & 31).astype(F32)
            both = jnp.concatenate([onehot * high, onehot * low], axis=0).astype(BF16)
            digits = digits + dot_nt(both, is_slot)
        requests = (digits[:nv] * 32.0 + digits[nv:]).astype(I32)
        for k in range(nv):
            reqo[k] = jnp.broadcast_to(requests[k : k + 1], reqo.shape[1:])
        reqi[nv - 1] = jnp.broadcast_to(requests[nv - 1 : nv], reqo.shape[1:])

    in_gain.wait()
    for n, u in enumerate((3, 2, 0, 1)):
        with scope(f"proj{n}"):
            in_lat[u].wait()
            wide = lat[u].astype(F32)
            mean_square = jnp.mean(wide * wide, axis=-1, keepdims=True)
            x = (wide * lax.rsqrt(mean_square + EPSILON) * gain[...]).astype(BF16)
            normed[u] = x
            if n == 0:
                in_k.wait()
            kv[2 + u, :tok, :] = dot(x, wqkv[1]).astype(BF16)
            if n == 0:
                in_v.wait()
            values = jnp.transpose(dot(x, wqkv[2])).astype(BF16)
            for h in range(sub // HEAD_DIM):
                top, first_row = value_rows(h)
                kv[2 + u, first_row : first_row + HEAD_DIM, :] = values[HEAD_DIM * h : HEAD_DIM * (h + 1)]
                if h % 2 == 0:
                    kv[2 + u, first_row + HEAD_DIM : first_row + HEAD_DIM + 16, :] = jnp.ones((16, tok), BF16)
        if n == 2:
            with scope("prep"):
                for copy in in_small:
                    copy.wait()
                prepare()
            with scope("greeted"):
                pl.semaphore_wait(barrier, nv + 1)
            for early in (0, 3, 2):
                kv_copy(early).start()
            in_wout.wait()
            for k in range(4):
                wo_copy(k).start()
    kv_copy(1).start()
    in_q.wait()
    def ask(begin, end):
        found = dot(normed[begin:end].reshape((end - begin) * tok, width), wqkv[0])
        found = (found * (HEAD_DIM ** (-0.5) * LOG2_E)).astype(BF16)
        q[begin:end] = found.reshape(end - begin, tok, sub)

    lane = lax.broadcasted_iota(I32, (1, 2 * HEAD_DIM), 1)
    first = lane < HEAD_DIM

    def attend(n, i):
        a = me * nl + actual(i)
        bias = []
        for j in range(5):
            d = j - 2
            if d == 0:
                bias.append(None)
            else:
                back = d * (1 - pc) if d > 0 else -d * pc
                source = lax.rem(a - back + views_total, views_total)
                present = inter[abs(d) - 1, source]
                bias.append((1.0 - present.astype(F32)) * 1e30)
        heads = sub // HEAD_DIM
        scores = []
        for h in range(heads):
            cols = slice(2 * HEAD_DIM * (h // 2), 2 * HEAD_DIM * (h // 2 + 1))
            both = q[i, :, cols]
            mine = first if h % 2 == 0 else jnp.logical_not(first)
            query = jnp.where(mine, both, jnp.zeros_like(both))
            tiles = []
            for j in range(5):
                s = dot_nt(kv[i + j, :tok, cols], query)
                high = jnp.max(s.reshape(tok // 8, 8, tok), axis=0)
                tiles.append((s, high if bias[j] is None else high - bias[j]))
            scores.append(tiles)
        for h in range(heads):
            top = functools.reduce(jnp.maximum, [high for _, high in scores[h]])
            top = jnp.max(top, axis=0, keepdims=True)
            found = None
            begin, _ = value_rows(h)
            for j in range(5):
                p = jnp.exp2(scores[h][j][0] - (top if bias[j] is None else top + bias[j]))
                part = dot(kv[i + j, begin : begin + HEAD_DIM + 16, :], p.astype(BF16))
                found = part if found is None else found + part
            if h % 2 == 0:
                numer, total = found[:HEAD_DIM], found[HEAD_DIM : HEAD_DIM + 1]
            else:
                numer, total = found[16:], found[0:1]
            turned[HEAD_DIM * h : HEAD_DIM * (h + 1), :] = numer / total
        att[n, 0] = jnp.transpose(turned[...]).astype(BF16)

    own, to_pair, to_opp = (
        pl.ds(pl.multiple_of(g * sub, sub), sub) for g in (z, pair, opp)
    )

    def rounded(a, b):
        return dot(a, b).astype(BF16).astype(F32)

    def pass_on(n):
        cols, block = ((to_pair, 3), (to_opp, 1))[n % 2]
        for c, part in pieces(n):
            att_copy(n, c, part).wait_recv()
            summed = rounded(att[n, 0, part], wout[:, cols]) + rounded(att[n, 1, part], wo[block])
            for f in (0, 1):
                part_s[f, n, part] = summed[:, halves[f]].astype(BF16)
            part_copy(n, 0, c, part).start()
            if n == 1:
                part_copy(n, 1, c, part).start()

    def lay_copy(n, f):
        here = pl.ds(pl.multiple_of(actual(ORDER[n]) * tok, tok), tok)
        return pltpu.make_async_copy(
            lay.at[f, here], lay_out.at[here, halves[f]], lay_sem.at[0]
        )

    def got_copy(c):
        here = pl.ds(c * tok, tok)
        return pltpu.make_async_copy(got.at[here], got_out.at[here], got_sem.at[0])

    def begin(n):
        proj = rounded(att[n, 0], wout[:, own]) + rounded(att[n, 1], wo[2 - 2 * (n % 2)])
        base[n] = proj

    def finish(n, f):
        u = ORDER[n]
        mine = pl.ds(pl.multiple_of(z * sub + f * fw, fw), fw)
        for c, part in pieces(n):
            part_copy(n, f, c, part).wait_recv()
        proj = base[n, :, halves[f]] + part_r[f, n].astype(F32)
        done = (lat[u, :, mine].astype(F32) + proj).astype(BF16)
        lay[f, pl.ds(pl.multiple_of(actual(u) * tok, tok), tok), :] = done
        lay_copy(n, f).start()

    n_slots = nv * cap

    def select_mine():
        places = jnp.transpose(idxs[...])
        for c in range(mb.shape[0]):
            at = places[:, c : c + 1].astype(I32)
            hit = at == lax.broadcasted_iota(I32, (lanes, n_slots), 1)
            fsel[lanes * c : lanes * (c + 1), :] = hit.astype(F32).astype(BF16)

    def select_asked():
        all_requests().wait()
        asked = jnp.transpose(reqi[:, 0, :])
        for k in range(nv):
            hit = asked[:cap, k : k + 1] == lax.broadcasted_iota(I32, (cap, nl * tok), 1)
            gsel[cap * k : cap * (k + 1), :] = hit.astype(F32).astype(BF16)

    for n, u in enumerate(ORDER):
        with scope(f"halo{n}"):
            kv_copy((0, 1, 3, 2)[n]).wait_recv()
        with scope(f"att{n}"):
            if n == 0:
                ask(0, nl)
            attend(n, u)
        for c, part in pieces(n):
            att_copy(n, c, part).start()
        if n == 1:
            for o in range(nv - 1):
                req_copy(o).start()
            for k in range(4):
                wo_copy(k).wait()
                wo_share(k).start()

    with scope("wo"):
        for k in range(4):
            wo_share(k).wait()
    with scope("pass1"):
        pass_on(1)
    with scope("pass0"):
        pass_on(0)
    with scope("sel_asked"):
        select_asked()
    with scope("pass2"):
        pass_on(2)
    with scope("pass3"):
        pass_on(3)
    for n in (0, 2, 3):
        for c, part in pieces(n):
            part_copy(n, 1, c, part).start()
    with scope("sel_mine"):
        select_mine()
    with scope("begin"):
        for n in range(nl):
            begin(n)

    for f in (0, 1):
        for n in range(nl):
            with scope(f"finish{f}{n}"):
                finish(n, f)
        for lo, hi in PICK_GROUPS:
            with scope(f"pick{f}{lo}"):
                picked = dot(gsel[cap * lo : cap * hi, :], lay[f]).astype(BF16)
                picked = picked.reshape(hi - lo, cap, fw)
                rows[f, lo:hi] = picked
                if hi == nv:
                    reps[f, nv - 1] = picked[-1]
                for o in range(lo, min(hi, nv - 1)):
                    rep_copy(f, o).start()

    for f in (0, 1):
        for lo, hi in TAKE_GROUPS:
            with scope(f"take{f}{lo}"):
                reply_group(f, lo // GROUP).wait()
                block = reps[f, lo:hi].reshape((hi - lo) * cap, fw)
                if hi < nv:
                    part = dot(fsel[:, cap * lo : cap * hi], block)
                    acc[...] = part if lo == 0 else acc[...] + part
                else:
                    for c in range(nl):
                        here = slice(c * tok, (c + 1) * tok)
                        part = dot(fsel[here, cap * lo : cap * hi], block)
                        got[here, halves[f]] = (acc[here, :] + part).astype(BF16)
                        if f == 1:
                            got_copy(c).start()

    with scope("sent"):
        for i in range(nl):
            kv_copy(i).wait_send()
            for c, part in pieces(i):
                att_copy(i, c, part).wait_send()
                for f in (0, 1):
                    part_copy(i, f, c, part).wait_send()
    with scope("stored"):
        pltpu.make_async_copy(got, lay_out, lay_sem.at[0]).wait()
        pltpu.make_async_copy(got, got_out, got_sem.at[0]).wait()


def blend(conf_h, lay_h, got_h, out_h, conf, lay, got, out, conf_sem, lay_sem, got_sem, out_sem):
    pieces, size, _ = lay.shape
    lanes = conf.shape[1]
    first = pltpu.make_async_copy(conf_h, conf, conf_sem.at[0])
    first.start()
    loads, stores = [], []
    for c in range(pieces):
        here = pl.ds(c * size, size)
        loads.append(
            (
                pltpu.make_async_copy(lay_h.at[here], lay.at[c], lay_sem.at[c]),
                pltpu.make_async_copy(got_h.at[here], got.at[c], got_sem.at[c]),
            )
        )
        stores.append(pltpu.make_async_copy(out.at[c], out_h.at[here], out_sem.at[c]))
        for copy in loads[c]:
            copy.start()
    first.wait()
    weight = COUPLING * jnp.transpose(conf[...])
    for c in range(pieces):
        for copy in loads[c]:
            copy.wait()
        for k in range(size // lanes):
            here = pl.ds(k * lanes, lanes)
            mine = lay[c, here].astype(F32)
            column = c * (size // lanes) + k
            other = got[c, here].astype(F32)
            out[c, here] = mine + weight[:, column : column + 1] * (other - mine)
        stores[c].start()
    for copy in stores:
        copy.wait()


def per_device(nv, latents, norm_gain, w_qkv, w_out, intersection, match_block, match_row, confidence):
    nl, tok, width = latents.shape
    sub = w_qkv.shape[2]
    rows = nl * tok
    cap = 2 * rows // nv
    here = pl.BlockSpec(memory_space=pltpu.HBM)
    dma = pltpu.SemaphoreType.DMA
    vmem = pltpu.VMEM
    lanes = 128
    lay, got = pl.pallas_call(
        functools.partial(kernel, nv, nl * nv, cap),
        out_shape=[jax.ShapeDtypeStruct((rows, sub), BF16)] * 2,
        in_specs=[here] * 7,
        out_specs=[here] * 2,
        scratch_shapes=[
            vmem((nl, tok, width), BF16),
            vmem((1, width), F32),
            vmem((3, width, sub), BF16),
            vmem((sub, width), BF16),
            pltpu.SMEM(intersection.shape[::-1], I32),
            vmem((rows // lanes, lanes), I32),
            vmem((rows // lanes, lanes), I32),
            vmem((nl + 4, 2 * tok + 32, sub), BF16),
            vmem((nl, tok, sub), BF16),
            vmem((nl, 2, tok, sub), BF16),
            vmem((4, sub, sub), BF16),
            vmem((2, nl, tok, sub // 2), BF16),
            vmem((2, nl, tok, sub // 2), BF16),
            vmem((2, rows, sub // 2), BF16),
            vmem((nv * cap, rows), BF16),
            vmem((rows, nv * cap), BF16),
            vmem((rows // lanes, lanes), F32),
            vmem((nv, 8, lanes), I32),
            vmem((nv, 8, lanes), I32),
            vmem((2, nv, cap, sub // 2), BF16),
            vmem((2, nv, cap, sub // 2), BF16),
            vmem((rows, sub // 2), F32),
            vmem((nl, tok, width), BF16),
            vmem((sub, tok), F32),
            vmem((rows, sub), BF16),
            vmem((nl, tok, sub), F32),
            dma((12,)), dma((1,)), dma((1,)),
            dma((nl,)), dma((nl,)), dma((4,)), dma((4,)), dma((4,)), dma((4,)),
            dma((nl + 1,)), dma((nl + 1,)), dma((2, nl + 1)), dma((2, nl + 1)),
            dma((1,)), dma((1,)), dma((2, nv // GROUP)), dma((2, nv // GROUP)),
        ],
        compiler_params=pltpu.CompilerParams(
            collective_id=0, has_side_effects=True, vmem_limit_bytes=VMEM_MIB * 1024 * 1024
        ),
    )(
        latents,
        norm_gain.reshape(1, width),
        w_qkv,
        w_out,
        intersection.T,
        match_block.reshape(rows // lanes, lanes),
        match_row.reshape(rows // lanes, lanes),
    )
    pieces = 4
    refined = pl.pallas_call(
        blend,
        out_shape=jax.ShapeDtypeStruct((rows, sub), F32),
        in_specs=[here] * 3,
        out_specs=here,
        scratch_shapes=[
            vmem((rows // lanes, lanes), F32),
            vmem((pieces, rows // pieces, sub), BF16),
            vmem((pieces, rows // pieces, sub), BF16),
            vmem((pieces, rows // pieces, sub), F32),
            dma((1,)), dma((pieces,)), dma((pieces,)), dma((pieces,)),
        ],
    )(confidence.reshape(rows // lanes, lanes), lay, got)
    return refined.reshape(nl, tok, sub)


def solution(mesh):
    in_specs = (
        P("views", None, None),
        P(),
        P(None, None, "heads"),
        P("heads", None),
        P(),
        P("views", None),
        P("views"),
        P("views"),
    )
    out_specs = P("views", None, "heads")
    return jax.shard_map(
        functools.partial(per_device, mesh.shape["views"]),
        mesh=mesh, in_specs=in_specs, out_specs=out_specs, check_vma=False,
    )
```

```python
import functools

import jax
import jax.numpy as jnp
from jax import lax
from jax.experimental import pallas as pl
from jax.experimental.pallas import tpu as pltpu
from jax.sharding import PartitionSpec as P

MESH = pl.DeviceIdType.MESH
F32, BF16, I32 = jnp.float32, jnp.bfloat16, jnp.int32
EPSILON = 1e-06
COUPLING = 0.5
LOG2_E = 1.4426950408889634
HEAD_DIM = 64
ORDER = (1, 0, 2, 3)
SIDE = 4
VMEM_MIB = 60


def ring_steps(d):
    return min(d, SIDE - d)


PLACES = sorted(
    ((dx, dy, dc) for dx in range(SIDE) for dy in range(SIDE) for dc in range(2)),
    key=lambda p: (-ring_steps(p[0]) - ring_steps(p[1]), -p[2]),
)
PICK_GROUPS = ((0, 4), (4, 8), (8, 16), (16, 24), (24, 32))
GROUP = 8
TAKE_GROUPS = ((0, 8), (8, 16), (16, 24), (24, 32))


def dot(a, b):
    return jnp.dot(a, b, preferred_element_type=F32)


def dot_nt(a, b):
    return lax.dot_general(a, b, (((1,), (1,)), ((), ())), preferred_element_type=F32)


def value_rows(h):
    start = 256 + (2 * HEAD_DIM + 16) * (h // 2) + (h % 2) * HEAD_DIM
    return start, start + 16 * (h % 2)


def scope(name):
    return jax.named_scope(name)


def kernel(
    nv, views_total, cap,
    lat_h, gain_h, wqkv_h, wout_h, inter_h, mb_h, mr_h,
    lay_out, got_out,
    lat, gain, wqkv, wout, inter, mb, mr,
    kv, q, att, wo, part_s, part_r, lay, gsel, fsel, idxs, reqo, reqi, rows, reps, acc, normed, turned, got, base,
    in_sem, lay_sem, got_sem, kv_s, kv_r, wo_s, wo_r, ws_s, ws_r, at_s, at_r, pt_s, pt_r, rq_s, rq_r, rp_s, rp_r,
):
    nl, tok, width = lat.shape
    sub = wqkv.shape[2]
    me = lax.axis_index("views")
    z = lax.axis_index("heads")
    odd = lax.rem(z, 2)
    pair, opp = z + 1 - 2 * odd, lax.rem(z + 3 + 2 * odd, 4)
    far = lax.rem(z + 2, 4)
    px, py, pc = me // (2 * SIDE), lax.rem(me // 2, SIDE), lax.rem(me, 2)
    partner = me + 1 - 2 * pc
    beyond = lax.rem(me + nv - 1 + 2 * pc, nv)

    def actual(u):
        return u * pc + (nl - 1 - u) * (1 - pc)

    def away(o, sign):
        dx, dy, dc = PLACES[o]
        bx = lax.rem(px + (dx if sign > 0 else SIDE - dx), SIDE)
        by = lax.rem(py + (dy if sign > 0 else SIDE - dy), SIDE)
        return bx * (2 * SIDE) + by * 2 + lax.rem(pc + dc, 2)

    def load(n, src, dst):
        copy = pltpu.make_async_copy(src, dst, in_sem.at[n])
        copy.start()
        return copy

    in_gain = load(0, gain_h, gain)
    in_lat = {3: load(1, lat_h.at[actual(3)], lat.at[3])}
    in_k = load(2, wqkv_h.at[1], wqkv.at[1])
    in_v = load(3, wqkv_h.at[2], wqkv.at[2])
    for u in (2, 0, 1):
        in_lat[u] = load(6 + u, lat_h.at[actual(u)], lat.at[u])
    in_wout = load(5, wout_h, wout)
    in_q = load(4, wqkv_h.at[0], wqkv.at[0])
    in_small = [load(9, mb_h, mb), load(10, mr_h, mr), load(11, inter_h, inter)]

    def remote(src, dst, send, recv, device):
        return pltpu.make_async_remote_copy(
            src_ref=src, dst_ref=dst, send_sem=send, recv_sem=recv,
            device_id=device, device_id_type=MESH,
        )

    barrier = pltpu.get_barrier_semaphore()

    def greet(k, carry):
        pl.semaphore_signal(
            barrier, inc=1, device_id=(lax.rem(me + k, nv), z), device_id_type=MESH
        )
        return carry

    lax.fori_loop(1, nv, greet, 0)
    for other in (pair, opp):
        pl.semaphore_signal(barrier, inc=1, device_id=(me, other), device_id_type=MESH)

    def kv_copy(u):
        slot = (1, 0, nl + 3, nl + 2)[u]
        target = partner if u < 2 else beyond
        return remote(kv.at[2 + u], kv.at[slot], kv_s.at[0], kv_r.at[u], (target, z))

    half = sub // 2
    my_half = pl.ds(pl.multiple_of(pc * half, half), half)

    def wo_copy(n):
        cols = pl.ds(pl.multiple_of((pair, far, opp, far)[n] * sub, sub), sub)
        target = (pair, opp)[n // 2]
        return remote(
            wout.at[my_half, cols], wo.at[n, my_half], wo_s.at[0], wo_r.at[0], (me, target)
        )

    def wo_share(n):
        block = wo.at[n, my_half]
        return remote(block, block, ws_s.at[0], ws_r.at[0], (partner, z))

    def ways(n):
        return (opp, pair) if n % 2 == 0 else (pair, opp)

    def pieces(n):
        size = tok // 2 if n == nl - 1 else tok
        return [(c, pl.ds(c * size, size)) for c in range(tok // size)]

    def att_copy(n, c, part):
        return remote(
            att.at[n, 0, part], att.at[n, 1, part], at_s.at[0], at_r.at[n + c], (me, ways(n)[0])
        )

    def part_copy(n, f, c, part):
        return remote(
            part_s.at[f, n, part], part_r.at[f, n, part],
            pt_s.at[0], pt_r.at[f, n + c], (me, ways(n)[1]),
        )

    def req_copy(o):
        return remote(reqo.at[o], reqi.at[o], rq_s.at[0], rq_r.at[0], (away(o, 1), z))

    def all_requests():
        here = pl.ds(0, nv - 1)
        return remote(reqo.at[here], reqi.at[here], rq_s.at[0], rq_r.at[0], (beyond, z))

    def rep_copy(f, o):
        g = o // GROUP
        return remote(
            rows.at[f, o], reps.at[f, o], rp_s.at[f, g], rp_r.at[f, g], (away(o, -1), z)
        )

    def reply_group(f, g):
        here = pl.ds(g * GROUP, min(GROUP, nv - 1 - g * GROUP))
        return remote(
            rows.at[f, here], reps.at[f, here], rp_s.at[f, g], rp_r.at[f, g], (beyond, z)
        )

    fw = sub // 2
    halves = (slice(0, fw), slice(fw, sub))

    lanes = mb.shape[1]

    def prepare():
        named = mb[...]
        rel = (((named >> 3) - px) & 3) * 8 + ((((named >> 1) & 3) - py) & 3) * 2 + ((named - pc) & 1)
        place = jnp.zeros_like(rel)
        for o, (dx, dy, dc) in enumerate(PLACES):
            place = jnp.where(rel == dx * 8 + dy * 2 + dc, o, place)
        wanted = mr[...]
        block_iota = lax.broadcasted_iota(I32, (nv, lanes), 0)
        slot_iota = lax.broadcasted_iota(I32, (lanes, lanes), 0)
        before = (slot_iota < lax.broadcasted_iota(I32, (lanes, lanes), 1)).astype(F32).astype(BF16)
        base = jnp.zeros((nv, 1), F32)
        digits = jnp.zeros((2 * nv, lanes), F32)
        for c in range(mb.shape[0]):
            onehot = (place[c : c + 1] == block_iota).astype(F32)
            earlier = dot(onehot.astype(BF16), before) + base
            slot = jnp.sum(onehot * earlier, axis=0, keepdims=True)
            base = base + jnp.sum(onehot, axis=1, keepdims=True)
            idxs[c : c + 1, :] = place[c : c + 1].astype(F32) * cap + slot
            is_slot = (slot.astype(I32) == slot_iota).astype(F32).astype(BF16)
            row = wanted[c : c + 1]
            high, low = (row >> 5).astype(F32), (row & 31).astype(F32)
            both = jnp.concatenate([onehot * high, onehot * low], axis=0).astype(BF16)
            digits = digits + dot_nt(both, is_slot)
        requests = (digits[:nv] * 32.0 + digits[nv:]).astype(I32)
        for k in range(nv):
            reqo[k] = jnp.broadcast_to(requests[k : k + 1], reqo.shape[1:])
        reqi[nv - 1] = jnp.broadcast_to(requests[nv - 1 : nv], reqo.shape[1:])

    in_gain.wait()
    for n, u in enumerate((3, 2, 0, 1)):
        with scope(f"proj{n}"):
            in_lat[u].wait()
            wide = lat[u].astype(F32)
            mean_square = jnp.mean(wide * wide, axis=-1, keepdims=True)
            x = (wide * lax.rsqrt(mean_square + EPSILON) * gain[...]).astype(BF16)
            normed[u] = x
            if n == 0:
                in_k.wait()
            kv[2 + u, :tok, :] = dot(x, wqkv[1]).astype(BF16)
            if n == 0:
                in_v.wait()
            values = jnp.transpose(dot(x, wqkv[2])).astype(BF16)
            for h in range(sub // HEAD_DIM):
                top, first_row = value_rows(h)
                kv[2 + u, first_row : first_row + HEAD_DIM, :] = values[HEAD_DIM * h : HEAD_DIM * (h + 1)]
                if h % 2 == 0:
                    kv[2 + u, first_row + HEAD_DIM : first_row + HEAD_DIM + 16, :] = jnp.ones((16, tok), BF16)
        if n == 2:
            with scope("prep"):
                for copy in in_small:
                    copy.wait()
                prepare()
            with scope("greeted"):
                pl.semaphore_wait(barrier, nv + 1)
            for early in (0, 3, 2):
                kv_copy(early).start()
            in_wout.wait()
            for k in range(4):
                wo_copy(k).start()
    kv_copy(1).start()
    in_q.wait()
    def ask(begin, end):
        found = dot(normed[begin:end].reshape((end - begin) * tok, width), wqkv[0])
        found = (found * (HEAD_DIM ** (-0.5) * LOG2_E)).astype(BF16)
        q[begin:end] = found.reshape(end - begin, tok, sub)

    lane = lax.broadcasted_iota(I32, (1, 2 * HEAD_DIM), 1)
    first = lane < HEAD_DIM

    def attend(n, i):
        a = me * nl + actual(i)
        bias = []
        for j in range(5):
            d = j - 2
            if d == 0:
                bias.append(None)
            else:
                back = d * (1 - pc) if d > 0 else -d * pc
                source = lax.rem(a - back + views_total, views_total)
                present = inter[abs(d) - 1, source]
                bias.append((1.0 - present.astype(F32)) * 1e30)
        heads = sub // HEAD_DIM
        scores = []
        for h in range(heads):
            cols = slice(2 * HEAD_DIM * (h // 2), 2 * HEAD_DIM * (h // 2 + 1))
            both = q[i, :, cols]
            mine = first if h % 2 == 0 else jnp.logical_not(first)
            query = jnp.where(mine, both, jnp.zeros_like(both))
            tiles = []
            for j in range(5):
                s = dot_nt(kv[i + j, :tok, cols], query)
                high = jnp.max(s.reshape(tok // 8, 8, tok), axis=0)
                tiles.append((s, high if bias[j] is None else high - bias[j]))
            scores.append(tiles)
        for h in range(heads):
            top = functools.reduce(jnp.maximum, [high for _, high in scores[h]])
            top = jnp.max(top, axis=0, keepdims=True)
            found = None
            begin, _ = value_rows(h)
            for j in range(5):
                p = jnp.exp2(scores[h][j][0] - (top if bias[j] is None else top + bias[j]))
                part = dot(kv[i + j, begin : begin + HEAD_DIM + 16, :], p.astype(BF16))
                found = part if found is None else found + part
            if h % 2 == 0:
                numer, total = found[:HEAD_DIM], found[HEAD_DIM : HEAD_DIM + 1]
            else:
                numer, total = found[16:], found[0:1]
            turned[HEAD_DIM * h : HEAD_DIM * (h + 1), :] = numer / total
        att[n, 0] = jnp.transpose(turned[...]).astype(BF16)

    own, to_pair, to_opp = (
        pl.ds(pl.multiple_of(g * sub, sub), sub) for g in (z, pair, opp)
    )

    def rounded(a, b):
        return dot(a, b).astype(BF16).astype(F32)

    def pass_on(n):
        cols, block = ((to_pair, 3), (to_opp, 1))[n % 2]
        for c, part in pieces(n):
            att_copy(n, c, part).wait_recv()
            summed = rounded(att[n, 0, part], wout[:, cols]) + rounded(att[n, 1, part], wo[block])
            for f in (0, 1):
                part_s[f, n, part] = summed[:, halves[f]].astype(BF16)
            part_copy(n, 0, c, part).start()
            if n == 1:
                part_copy(n, 1, c, part).start()

    def lay_copy(n, f):
        here = pl.ds(pl.multiple_of(actual(ORDER[n]) * tok, tok), tok)
        return pltpu.make_async_copy(
            lay.at[f, here], lay_out.at[here, halves[f]], lay_sem.at[0]
        )

    def got_copy(c):
        here = pl.ds(c * tok, tok)
        return pltpu.make_async_copy(got.at[here], got_out.at[here], got_sem.at[0])

    def begin(n):
        proj = rounded(att[n, 0], wout[:, own]) + rounded(att[n, 1], wo[2 - 2 * (n % 2)])
        base[n] = proj

    def finish(n, f):
        u = ORDER[n]
        mine = pl.ds(pl.multiple_of(z * sub + f * fw, fw), fw)
        for c, part in pieces(n):
            part_copy(n, f, c, part).wait_recv()
        proj = base[n, :, halves[f]] + part_r[f, n].astype(F32)
        done = (lat[u, :, mine].astype(F32) + proj).astype(BF16)
        lay[f, pl.ds(pl.multiple_of(actual(u) * tok, tok), tok), :] = done
        lay_copy(n, f).start()

    n_slots = nv * cap

    def select_mine():
        places = jnp.transpose(idxs[...])
        for c in range(mb.shape[0]):
            at = places[:, c : c + 1].astype(I32)
            hit = at == lax.broadcasted_iota(I32, (lanes, n_slots), 1)
            fsel[lanes * c : lanes * (c + 1), :] = hit.astype(F32).astype(BF16)

    def select_asked():
        all_requests().wait()
        asked = jnp.transpose(reqi[:, 0, :])
        for k in range(nv):
            hit = asked[:cap, k : k + 1] == lax.broadcasted_iota(I32, (cap, nl * tok), 1)
            gsel[cap * k : cap * (k + 1), :] = hit.astype(F32).astype(BF16)

    for n, u in enumerate(ORDER):
        with scope(f"halo{n}"):
            kv_copy((0, 1, 3, 2)[n]).wait_recv()
        with scope(f"att{n}"):
            if n == 0:
                ask(0, nl)
            attend(n, u)
        for c, part in pieces(n):
            att_copy(n, c, part).start()
        if n == 1:
            for o in range(nv - 1):
                req_copy(o).start()
            blocks = wo.at[:, my_half]
            remote(blocks, blocks, wo_s.at[0], wo_r.at[0], (me, pair)).wait()
            for k in range(4):
                wo_share(k).start()

    with scope("wo"):
        blocks = wo.at[:, my_half]
        remote(blocks, blocks, ws_s.at[0], ws_r.at[0], (partner, z)).wait()
    with scope("pass1"):
        pass_on(1)
    with scope("pass0"):
        pass_on(0)
    with scope("sel_asked"):
        select_asked()
    with scope("pass2"):
        pass_on(2)
    with scope("pass3"):
        pass_on(3)
    for n in (0, 2, 3):
        for c, part in pieces(n):
            part_copy(n, 1, c, part).start()
    with scope("sel_mine"):
        select_mine()
    with scope("begin"):
        for n in range(nl):
            begin(n)

    for f in (0, 1):
        for n in range(nl):
            with scope(f"finish{f}{n}"):
                finish(n, f)
        for lo, hi in PICK_GROUPS:
            with scope(f"pick{f}{lo}"):
                picked = dot(gsel[cap * lo : cap * hi, :], lay[f]).astype(BF16)
                picked = picked.reshape(hi - lo, cap, fw)
                rows[f, lo:hi] = picked
                if hi == nv:
                    reps[f, nv - 1] = picked[-1]
                for o in range(lo, min(hi, nv - 1)):
                    rep_copy(f, o).start()

    for f in (0, 1):
        for lo, hi in TAKE_GROUPS:
            with scope(f"take{f}{lo}"):
                reply_group(f, lo // GROUP).wait()
                block = reps[f, lo:hi].reshape((hi - lo) * cap, fw)
                if hi < nv:
                    part = dot(fsel[:, cap * lo : cap * hi], block)
                    acc[...] = part if lo == 0 else acc[...] + part
                else:
                    for c in range(nl):
                        here = slice(c * tok, (c + 1) * tok)
                        part = dot(fsel[here, cap * lo : cap * hi], block)
                        got[here, halves[f]] = (acc[here, :] + part).astype(BF16)
                        if f == 1:
                            got_copy(c).start()

    with scope("sent"):
        here = pl.ds(2, nl)
        remote(kv.at[here], kv.at[here], kv_s.at[0], kv_r.at[0], (partner, z)).wait_send()
        remote(att.at[:, 0], att.at[:, 0], at_s.at[0], at_r.at[0], (me, pair)).wait_send()
        remote(part_s, part_s, pt_s.at[0], pt_r.at[0, 0], (me, pair)).wait_send()
    with scope("stored"):
        pltpu.make_async_copy(got, lay_out, lay_sem.at[0]).wait()
        pltpu.make_async_copy(got, got_out, got_sem.at[0]).wait()


def blend(conf_h, lay_h, got_h, out_h, conf, lay, got, out, conf_sem, lay_sem, got_sem, out_sem):
    pieces, size, _ = lay.shape
    lanes = conf.shape[1]
    first = pltpu.make_async_copy(conf_h, conf, conf_sem.at[0])
    first.start()
    loads, stores = [], []
    for c in range(pieces):
        here = pl.ds(c * size, size)
        loads.append(
            (
                pltpu.make_async_copy(lay_h.at[here], lay.at[c], lay_sem.at[c]),
                pltpu.make_async_copy(got_h.at[here], got.at[c], got_sem.at[c]),
            )
        )
        stores.append(pltpu.make_async_copy(out.at[c], out_h.at[here], out_sem.at[c]))
        for copy in loads[c]:
            copy.start()
    first.wait()
    weight = COUPLING * jnp.transpose(conf[...])
    for c in range(pieces):
        for copy in loads[c]:
            copy.wait()
        for k in range(size // lanes):
            here = pl.ds(k * lanes, lanes)
            mine = lay[c, here].astype(F32)
            column = c * (size // lanes) + k
            other = got[c, here].astype(F32)
            out[c, here] = mine + weight[:, column : column + 1] * (other - mine)
        stores[c].start()
    for copy in stores:
        copy.wait()


def per_device(nv, latents, norm_gain, w_qkv, w_out, intersection, match_block, match_row, confidence):
    nl, tok, width = latents.shape
    sub = w_qkv.shape[2]
    rows = nl * tok
    cap = 2 * rows // nv
    here = pl.BlockSpec(memory_space=pltpu.HBM)
    dma = pltpu.SemaphoreType.DMA
    vmem = pltpu.VMEM
    lanes = 128
    lay, got = pl.pallas_call(
        functools.partial(kernel, nv, nl * nv, cap),
        out_shape=[jax.ShapeDtypeStruct((rows, sub), BF16)] * 2,
        in_specs=[here] * 7,
        out_specs=[here] * 2,
        scratch_shapes=[
            vmem((nl, tok, width), BF16),
            vmem((1, width), F32),
            vmem((3, width, sub), BF16),
            vmem((sub, width), BF16),
            pltpu.SMEM(intersection.shape[::-1], I32),
            vmem((rows // lanes, lanes), I32),
            vmem((rows // lanes, lanes), I32),
            vmem((nl + 4, 2 * tok + 32, sub), BF16),
            vmem((nl, tok, sub), BF16),
            vmem((nl, 2, tok, sub), BF16),
            vmem((4, sub, sub), BF16),
            vmem((2, nl, tok, sub // 2), BF16),
            vmem((2, nl, tok, sub // 2), BF16),
            vmem((2, rows, sub // 2), BF16),
            vmem((nv * cap, rows), BF16),
            vmem((rows, nv * cap), BF16),
            vmem((rows // lanes, lanes), F32),
            vmem((nv, 8, lanes), I32),
            vmem((nv, 8, lanes), I32),
            vmem((2, nv, cap, sub // 2), BF16),
            vmem((2, nv, cap, sub // 2), BF16),
            vmem((rows, sub // 2), F32),
            vmem((nl, tok, width), BF16),
            vmem((sub, tok), F32),
            vmem((rows, sub), BF16),
            vmem((nl, tok, sub), F32),
            dma((12,)), dma((1,)), dma((1,)),
            dma((1,)), dma((nl,)), dma((1,)), dma((1,)), dma((1,)), dma((1,)),
            dma((1,)), dma((nl + 1,)), dma((1,)), dma((2, nl + 1)),
            dma((1,)), dma((1,)), dma((2, nv // GROUP)), dma((2, nv // GROUP)),
        ],
        compiler_params=pltpu.CompilerParams(
            collective_id=0, has_side_effects=True, vmem_limit_bytes=VMEM_MIB * 1024 * 1024
        ),
    )(
        latents,
        norm_gain.reshape(1, width),
        w_qkv,
        w_out,
        intersection.T,
        match_block.reshape(rows // lanes, lanes),
        match_row.reshape(rows // lanes, lanes),
    )
    pieces = 4
    refined = pl.pallas_call(
        blend,
        out_shape=jax.ShapeDtypeStruct((rows, sub), F32),
        in_specs=[here] * 3,
        out_specs=here,
        scratch_shapes=[
            vmem((rows // lanes, lanes), F32),
            vmem((pieces, rows // pieces, sub), BF16),
            vmem((pieces, rows // pieces, sub), BF16),
            vmem((pieces, rows // pieces, sub), F32),
            dma((1,)), dma((pieces,)), dma((pieces,)), dma((pieces,)),
        ],
    )(confidence.reshape(rows // lanes, lanes), lay, got)
    return refined.reshape(nl, tok, sub)


def solution(mesh):
    in_specs = (
        P("views", None, None),
        P(),
        P(None, None, "heads"),
        P("heads", None),
        P(),
        P("views", None),
        P("views"),
        P("views"),
    )
    out_specs = P("views", None, "heads")
    return jax.shard_map(
        functools.partial(per_device, mesh.shape["views"]),
        mesh=mesh, in_specs=in_specs, out_specs=out_specs, check_vma=False,
    )
```
